32 devices in a mesh: gx: 4 (over y, core), gy: 8 (over z, x).
Axes of the slice: x: 2, y: 2, z: 4, core: 2. Of those that a mesh axis runs over, the one named last changes fastest.
Arguments:
- offsets: float32 [2, 8, 64, 128], P(None, 'gx', 'gy'), may hold values from 0 to 1
- masses: float32 [8, 64, 128], P('gx', 'gy'), may hold values from 0.01 to 0.04
- counts: int32 [8, 64], P('gx', 'gy'), may hold values from 1 to 128, as said below
- source: float32 [8, 64, 128], P('gx', 'gy'), may hold values from -6 to 6
Outputs:
- density: float32 [8, 64, 128], P('gx', 'gy')
- pressure: float32 [8, 64, 128], P('gx', 'gy')
- residual: float32 [8, 64, 128], P('gx', 'gy')
- peaks: float32 [5], replicated
The draws below stay inside these ranges and needn't reach their ends.
Inputs may be any that keep to these rules, and one draw needn't show every extreme that they name: `counts`: each cell's occupied slots come first; some cell holds 128 particles.
All inputs are finite; a program needn't handle non-finite values.
Results may differ from the reference program's by a relative error of at most 0.0003.
Values sent between devices are 32-bit elements; how exact they have to be, the bound alone decides.
A program may use at most 64 MiB of HBM per device.

```python
import math
import jax
import jax.numpy as jnp
from jax import lax

SLOT = 128
ITERS = 5
NX = 8
NY = 64


def draw_counts(key, part):
    coarse_key = jax.random.fold_in(key, 11)
    fine_key = jax.random.fold_in(key, 12)
    region_rows = (NX + 3) // 4
    region_cols = (NY + 3) // 4
    floor_count = jax.random.randint(coarse_key, (region_rows, region_cols), 1, SLOT + 1)
    floor_count = jnp.repeat(jnp.repeat(floor_count, 4, axis=0), 4, axis=1)[:NX, :NY]
    counts = jax.random.randint(fine_key, (NX, NY), floor_count, SLOT + 1)
    return counts.at[0, 0].set(SLOT).astype(jnp.int32)


def draw_source(key, part):
    rough = jnp.clip(jax.random.normal(jax.random.fold_in(key, 21), (NX, NY, SLOT), jnp.float32), -6.0, 6.0)
    return rough


def level_of(key, dims, cuts, least, top_value):
    def one(dim, parts):
        steps = jax.random.uniform(jax.random.fold_in(jax.random.fold_in(key, 6), dim), (parts,), jnp.float32, least / len(cuts), top_value / len(cuts))
        return jnp.repeat(jnp.exp(steps), dims[dim] // parts).reshape((-1,) + (1,) * (len(dims) - dim - 1))

    level = one(*cuts[0])
    for cut in cuts[1:]:
        level = level * one(*cut)
    return level


def setup_inputs(seed: int = 0) -> dict:
    key_list = jax.random.split(jax.random.key(seed), 5)
    return {
        "offsets": jnp.clip(1.0 * jax.random.uniform(key_list[0], (2, NX, NY, SLOT), jnp.float32) ** level_of(key_list[0], (2, NX, NY, SLOT), ((1, 4), (2, 8)), -0.2, 0.2), 0.0, 1.0),
        "masses": jnp.clip(jnp.exp(math.log(0.04) - 1.3862944 * jax.random.uniform(key_list[1], (NX, NY, SLOT), jnp.float32) ** level_of(key_list[1], (NX, NY, SLOT), ((0, 4), (1, 8)), -0.2, 0.2)), 0.01, 0.04),
        "counts": draw_counts(jax.random.fold_in(key_list[4], 71), 0),
        "source": draw_source(jax.random.fold_in(key_list[4], 71), 0),
    }


BASE_STIFF = 0.5
PAIR_SCALE = 0.05
NEIGHBOUR_STEPS = [(step_x, step_y) for step_x in (-1, 0, 1) for step_y in (-1, 0, 1)]


def near_view(padded, step_x, step_y):
    row_count = padded.shape[-3] - 2
    col_count = padded.shape[-2] - 2
    return padded[..., 1 + step_x:1 + step_x + row_count, 1 + step_y:1 + step_y + col_count, :]


def kernel_terms(own_cells, nearby, step_x, step_y):
    offset_x = (step_x + nearby[0][..., None, :]) - own_cells[0][..., :, None]
    offset_y = (step_y + nearby[1][..., None, :]) - own_cells[1][..., :, None]
    return jnp.maximum(1.0 - (offset_x * offset_x + offset_y * offset_y), 0.0)


def density_block(padded):
    own_cells = near_view(padded, 0, 0)
    summed = jnp.zeros(own_cells.shape[1:], jnp.float32)
    for step_x, step_y in NEIGHBOUR_STEPS:
        nearby = near_view(padded, step_x, step_y)
        falloff = kernel_terms(own_cells, nearby, step_x, step_y)
        summed = summed + jnp.sum(falloff * falloff * falloff * nearby[2][..., None, :], axis=-1)
    return 1.0 + summed


def pair_weights(padded, step_x, step_y):
    own_cells = near_view(padded, 0, 0)
    nearby = near_view(padded, step_x, step_y)
    falloff = kernel_terms(own_cells, nearby, step_x, step_y)
    pairing = own_cells[3][..., :, None] * nearby[3][..., None, :] * (2.0 * PAIR_SCALE) / (own_cells[4][..., :, None] + nearby[4][..., None, :])
    return falloff * falloff * pairing


def diag_block(padded):
    own_cells = near_view(padded, 0, 0)
    summed = jnp.zeros(own_cells.shape[1:], jnp.float32)
    for step_x, step_y in NEIGHBOUR_STEPS:
        summed = summed + jnp.sum(pair_weights(padded, step_x, step_y), axis=-1)
    return BASE_STIFF + summed


def apply_block(padded, padded_field):
    own_cells = near_view(padded, 0, 0)
    summed = jnp.zeros(own_cells.shape[1:], jnp.float32)
    for step_x, step_y in NEIGHBOUR_STEPS:
        summed = summed + jnp.einsum('xyij,xyj->xyi', pair_weights(padded, step_x, step_y), near_view(padded_field, step_x, step_y), precision=lax.Precision.HIGHEST)
    return summed


def reference(offsets, masses, counts, source):
    slot_count = offsets.shape[-1]
    occupied = (jnp.arange(slot_count, dtype=jnp.int32)[None, None, :] < counts[:, :, None]).astype(jnp.float32)
    fields = jnp.stack([offsets[0], offsets[1], masses * occupied, occupied])
    padded = jnp.pad(fields, ((0, 0), (1, 1), (1, 1), (0, 0)))
    row_ids = jnp.arange(fields.shape[1], dtype=jnp.int32)
    density = lax.map(lambda row_index: density_block(lax.dynamic_slice_in_dim(padded, row_index, 3, 1))[0], row_ids)
    full = jnp.concatenate([padded, jnp.pad(density, ((1, 1), (1, 1), (0, 0)))[None]], 0)
    diagonal = lax.map(lambda row_index: diag_block(lax.dynamic_slice_in_dim(full, row_index, 3, 1))[0], row_ids)

    def operate(vector):
        padded_field = jnp.pad(vector, ((1, 1), (1, 1), (0, 0)))
        sums = lax.map(lambda row_index: apply_block(lax.dynamic_slice_in_dim(full, row_index, 3, 1), lax.dynamic_slice_in_dim(padded_field, row_index, 3, 0))[0], row_ids)
        return diagonal * vector - sums

    pressure = jnp.zeros_like(source)
    residual = source * occupied
    scaled = residual / diagonal
    direction = scaled
    precond_now = jnp.sum(residual * scaled)
    peak_list = []
    for step in range(ITERS):
        image = operate(direction)
        step_size = precond_now / jnp.sum(direction * image)
        pressure = pressure + step_size * direction
        residual = residual - step_size * image
        peak_list.append(jnp.max(jnp.abs(residual)))
        scaled = residual / diagonal
        precond_next = jnp.sum(residual * scaled)
        direction = scaled + (precond_next / precond_now) * direction
        precond_now = precond_next
    return density, pressure, residual, jnp.stack(peak_list)
```

```python
import functools

import jax
import jax.numpy as jnp
from jax import lax
from jax.experimental import pallas as pl
from jax.experimental.pallas import tpu as pltpu
from jax.sharding import PartitionSpec as P

ITERS = 5
BASE_STIFF = 0.5
PAIR_SCALE = 0.05
NEIGHBOUR_STEPS = [(step_x, step_y) for step_x in (-1, 0, 1) for step_y in (-1, 0, 1)]
SIDES = [step for step in NEIGHBOUR_STEPS if step != (0, 0)]
MESH = pl.DeviceIdType.MESH
FAR = 64.0
CENTRE, HALF = 0.4375, 0.5
CHUNK = 64


def two_sum(a, b):
    total = a + b
    part = total - a
    return total, (a - (total - part)) + (b - part)


def add(a, b):
    high, low = two_sum(a[0], b[0])
    return high, low + (a[1] + b[1])


def tidy(a):
    high = a[0] + a[1]
    return high, a[1] - (high - a[0])


def halves(a):
    wide = a * 4097.0
    high = wide - (wide - a)
    return high, a - high


def mul(a, b):
    a_high, a_low = halves(a[0])
    b_high, b_low = halves(b[0])
    product = a[0] * b[0]
    rest = ((a_high * b_high - product) + (a_high * b_low + a_low * b_high)) + a_low * b_low
    return tidy((product, rest + (a[0] * b[1] + a[1] * b[0])))


def neg(a):
    return -a[0], -a[1]


def sub(a, b):
    return tidy(add(a, neg(b)))


def inverse(a):
    first = 1.0 / a[0]
    start = (first, jnp.zeros_like(first))
    one = (jnp.ones_like(first), jnp.zeros_like(first))
    rest = sub(one, mul(start, a))
    return tidy((first, rest[0] * first))


def tree(items, combine):
    items = list(items)
    while len(items) > 1:
        paired = [combine(items[at], items[at + 1]) for at in range(0, len(items) - 1, 2)]
        items = paired + items[len(paired) * 2 :]
    return items[0]


def over_sublanes(pair, rows):
    shift = rows // 2
    while shift:
        pair = add(pair, tuple(pltpu.roll(part, shift, 0) for part in pair))
        shift //= 2
    return pair


def kernel(
    size_x, size_y, row_count, col_count,
    offsets_hbm, masses_hbm, counts_hbm, source_hbm,
    density_ref, pressure_ref, residual_ref, peaks_ref,
    offsets_ref, masses_ref, counts_ref, source_ref, load_sem,
    pad_fields, pad_density, pad_vector, weights, own_x, own_y, own_density,
    part, inverse_diag, diag_ref, vectors, products, images,
    gather_early, gather_late, gather_peak,
    field_send, field_recv, density_send, density_recv, vector_send, vector_recv,
    early_send, early_recv, late_send, late_recv, peak_send, peak_recv,
):
    here_x, here_y = lax.axis_index("gx"), lax.axis_index("gy")
    device_count = size_x * size_y
    slots = masses_ref.shape[-1]

    loads = [
        pltpu.make_async_copy(source, target, load_sem.at[index])
        for index, (source, target) in enumerate((
            (offsets_hbm, offsets_ref), (masses_hbm, masses_ref),
            (counts_hbm, counts_ref), (source_hbm, source_ref),
        ))
    ]
    for load in loads:
        load.start()

    low_x, high_x = (here_x > 0), (here_x < size_x - 1)
    low_y, high_y = (here_y > 0), (here_y < size_y - 1)

    def on_side(step_x, step_y, action):
        conditions = []
        if step_x:
            conditions.append({1: high_x, -1: low_x}[step_x])
        if step_y:
            conditions.append({1: high_y, -1: low_y}[step_y])
        condition = conditions[0]
        for other in conditions[1:]:
            condition = jnp.logical_and(condition, other)
        pl.when(condition)(action)

    def ahead(here, step, size):
        there = here + step
        return jnp.where(there >= size, there - size, there)

    def for_peers(action):
        if device_count <= 64:
            for index in range(1, device_count):
                action(index, index // size_y, index % size_y)
        else:
            def one(index, carry):
                action(index, lax.div(index, size_y), lax.rem(index, size_y))
                return carry

            lax.fori_loop(1, device_count, one, 0)

    barrier = pltpu.get_barrier_semaphore()

    def greet(device):
        pl.semaphore_signal(barrier, inc=1, device_id=device, device_id_type=MESH)

    near_only = max(size_x, size_y) <= ITERS + 3
    if near_only:
        for step_x, step_y in SIDES:
            on_side(step_x, step_y, functools.partial(greet, (here_x + step_x, here_y + step_y)))
    else:
        for_peers(lambda index, step_x, step_y: greet(
            (ahead(here_x, step_x, size_x), ahead(here_y, step_y, size_y))
        ))

    def fill(ref, value):
        ref[...] = jnp.full(ref.shape, value, jnp.float32)

    def fill_outside(at):
        fill(pad_fields.at[at], FAR)
        fill(pad_density.at[at], 0.0)
        for step in range(ITERS):
            fill(pad_vector.at[(step,) + at], 0.0)

    every = slice(None)
    pl.when(jnp.logical_not(low_x))(lambda: fill_outside((0, every)))
    pl.when(jnp.logical_not(high_x))(lambda: fill_outside((row_count + 1, every)))
    pl.when(jnp.logical_not(low_y))(lambda: fill_outside((every, 0)))
    pl.when(jnp.logical_not(high_y))(lambda: fill_outside((every, col_count + 1)))

    def halo_copy(side, pad, send_sem, recv_sem):
        step_x, step_y = SIDES[side]
        inner = lambda step, count: {1: pl.ds(count, 1), -1: pl.ds(1, 1), 0: pl.ds(1, count)}[step]
        outer = lambda step, count: {1: pl.ds(0, 1), -1: pl.ds(count + 1, 1), 0: pl.ds(1, count)}[step]
        return pltpu.make_async_remote_copy(
            src_ref=pad.at[inner(step_x, row_count), inner(step_y, col_count)],
            dst_ref=pad.at[outer(step_x, row_count), outer(step_y, col_count)],
            send_sem=send_sem.at[side],
            recv_sem=recv_sem.at[side],
            device_id=(here_x + step_x, here_y + step_y),
            device_id_type=MESH,
        )

    LONG = [side for side, step in enumerate(SIDES) if step[1]]
    SHORT = [side for side, step in enumerate(SIDES) if not step[1]]

    def start_halo(sides, *args):
        for side in sides:
            on_side(*SIDES[side], lambda side=side: halo_copy(side, *args).start())

    def end_halo(*args):
        for side, (step_x, step_y) in enumerate(SIDES):
            on_side(-step_x, -step_y, lambda side=side: halo_copy(side, *args).wait_recv())

    def end_sends(*args):
        for side, (step_x, step_y) in enumerate(SIDES):
            on_side(step_x, step_y, lambda side=side: halo_copy(side, *args).wait_send())

    def steps_of(row, place, inside):
        def is_inside(step_x, step_y):
            if not 0 <= row + step_x < row_count:
                return False
            return not (place == "first" and step_y < 0 or place == "last" and step_y > 0)

        return [
            (index, step_x, step_y)
            for index, (step_x, step_y) in enumerate(NEIGHBOUR_STEPS)
            if is_inside(step_x, step_y) == inside
        ]

    def edge_columns(action):
        for col, place in ((0, "first"), (col_count - 1, "last")):
            for row in range(row_count):
                action(row, col, place)

    def inner_columns(action):
        def one(col, carry):
            for row in range(row_count):
                action(row, col, "inner")
            return carry

        lax.fori_loop(1, col_count - 1, one, 0)

    def all_columns(action):
        edge_columns(action)
        inner_columns(action)

    def spread(row):
        return jnp.broadcast_to(row, (slots, slots)).T

    def gathered(total):
        return jnp.sum(total.T, axis=0, keepdims=True)

    def chunks(terms):
        return gathered(jnp.concatenate(
            [terms(pl.ds(start, CHUNK)) for start in range(0, slots, CHUNK)], axis=0
        ))

    for load in loads:
        load.wait()
    lane = lax.broadcasted_iota(jnp.int32, (col_count, slots), 1)
    square = (col_count, col_count)
    on_diagonal = lax.broadcasted_iota(jnp.int32, square, 0) == lax.broadcasted_iota(jnp.int32, square, 1)
    occupied = []
    for row in range(row_count):
        limits = jnp.where(
            on_diagonal, jnp.broadcast_to(counts_ref[row : row + 1].astype(jnp.float32), square), 0.0
        )
        limit = jnp.sum(limits, axis=1, keepdims=True)
        occupied.append((lane.astype(jnp.float32) < limit).astype(jnp.float32))
        live = occupied[row] > 0.0
        field_rows = (
            jnp.where(live, offsets_ref[0, row], FAR),
            jnp.where(live, offsets_ref[1, row], FAR),
            masses_ref[row],
            source_ref[row] * occupied[row],
        )
        source_ref[row] = field_rows[3]
        for col in range(col_count):
            for index in range(3):
                pad_fields[row + 1, col + 1, index : index + 1] = field_rows[index][col : col + 1]
        inverse_diag[row] = occupied[row].reshape(col_count, 1, slots)

    def spread_place(row, col, place):
        own_x[row, col] = spread(offsets_ref[0, row, pl.ds(col, 1)])
        own_y[row, col] = spread(offsets_ref[1, row, pl.ds(col, 1)])

    all_columns(spread_place)

    greeters = lambda low, high: low.astype(jnp.int32) + high.astype(jnp.int32)
    if near_only:
        count_x, count_y = greeters(low_x, high_x), greeters(low_y, high_y)
        pl.semaphore_wait(barrier, (count_x + 1) * (count_y + 1) - 1)
    else:
        pl.semaphore_wait(barrier, device_count - 1)

    field_args = (pad_fields, field_send, field_recv)
    start_halo(range(len(SIDES)), *field_args)

    def density_part(inside):
        def one(row, col, place):
            steps = steps_of(row, place, inside)

            def terms(rows):
                at_x, at_y = own_x[row, col, rows], own_y[row, col, rows]
                total = None
                for index, step_x, step_y in steps:
                    near = pad_fields[row + 1 + step_x, col + 1 + step_y]
                    offset_x = (step_x + near[0:1]) - at_x
                    offset_y = (step_y + near[1:2]) - at_y
                    falloff = jnp.maximum(1.0 - (offset_x * offset_x + offset_y * offset_y), 0.0)
                    squared = falloff * falloff
                    weights[row, col, index, rows] = squared
                    term = squared * falloff * near[2:3]
                    total = term if total is None else total + term
                return total

            return chunks(terms)

        return one

    def store_density_part(row, col, place):
        part[row, col] = density_part(True)(row, col, place)

    all_columns(store_density_part)
    end_halo(*field_args)

    def finish_density(row, col, place):
        density = 1.0 + (part[row, col] + density_part(False)(row, col, place))
        pad_density[row + 1, col + 1] = density
        density_ref[row, pl.ds(col, 1)] = density

    density_args = (pad_density, density_send, density_recv)
    edge_columns(finish_density)
    start_halo(LONG, *density_args)
    inner_columns(finish_density)
    start_halo(SHORT, *density_args)

    def weight_part(inside):
        def one(row, col, place):
            steps = steps_of(row, place, inside)

            def terms(rows):
                here = own_density[row, col, rows]
                total = None
                for index, step_x, step_y in steps:
                    there = pad_density[row + 1 + step_x, col + 1 + step_y]
                    weight = weights[row, col, index, rows] * ((2.0 * PAIR_SCALE) / (here + there))
                    weights[row, col, index, rows] = weight
                    total = weight if total is None else total + weight
                return total

            return chunks(terms)

        return one

    def store_weight_part(row, col, place):
        own_density[row, col] = spread(pad_density[row + 1, col + 1])
        part[row, col] = weight_part(True)(row, col, place)

    all_columns(store_weight_part)
    end_halo(*density_args)

    def finish_weights(row, col, place):
        occupied_row = inverse_diag[row, col]
        total = part[row, col] + weight_part(False)(row, col, place)
        diagonal = BASE_STIFF + occupied_row * total
        inverted = occupied_row / diagonal
        scaled = source_ref[row, pl.ds(col, 1)] * inverted
        diag_ref[row, pl.ds(col, 1)] = diagonal
        inverse_diag[row, col] = inverted
        vectors[0, row, pl.ds(col, 1)] = scaled
        pad_vector[0, row + 1, col + 1] = scaled

    def vector_args(step):
        return pad_vector.at[step], vector_send.at[step], vector_recv.at[step]

    edge_columns(finish_weights)
    start_halo(LONG, *vector_args(0))
    inner_columns(finish_weights)
    start_halo(SHORT, *vector_args(0))

    def product_part(step, inside):
        def one(row, col, place):
            total = None
            for index, step_x, step_y in steps_of(row, place, inside):
                term = weights[row, col, index] * pad_vector[step, row + 1 + step_x, col + 1 + step_y]
                total = term if total is None else total + term
            return gathered(total)

        return one

    def store_product_part(step):
        def one(row, col, place):
            part[row, col] = product_part(step, True)(row, col, place)

        return one

    def finish_product(step):
        def one(row, col, place):
            product = part[row, col] + product_part(step, False)(row, col, place)
            products[step, row, pl.ds(col, 1)] = product
            now = vectors[step, row, pl.ds(col, 1)]
            rest = inverse_diag[row, col] * product - CENTRE * now
            if step == 0:
                following = rest * (1.0 / HALF)
            else:
                following = rest * (2.0 / HALF) - vectors[step - 1, row, pl.ds(col, 1)]
            vectors[step + 1, row, pl.ds(col, 1)] = following
            if step + 1 < ITERS:
                pad_vector[step + 1, row + 1, col + 1] = following

        return one

    def set_image(step):
        for row in range(row_count):
            images[step, row] = diag_ref[row] * vectors[step, row] - products[step, row]

    def dot(left, right):
        zero = jnp.zeros((col_count, slots), jnp.float32)
        return tree([(left[row] * right[row], zero) for row in range(row_count)], add)

    def send_all(gather, send_sem, recv_sem):
        def one(index, step_x, step_y):
            return pltpu.make_async_remote_copy(
                src_ref=gather.at[0],
                dst_ref=gather.at[index],
                send_sem=send_sem.at[index],
                recv_sem=recv_sem.at[index],
                device_id=(ahead(here_x, step_x, size_x), ahead(here_y, step_y, size_y)),
                device_id_type=MESH,
            )

        return one

    def start_all(*args):
        for_peers(lambda *peer: send_all(*args)(*peer).start())

    def end_all(*args):
        for_peers(lambda *peer: send_all(*args)(*peer).wait_recv())

    def end_all_sends(*args):
        for_peers(lambda *peer: send_all(*args)(*peer).wait_send())

    early_args = (gather_early, early_send, early_recv)
    late_args = (gather_late, late_send, late_recv)
    peak_args = (gather_peak, peak_send, peak_recv)
    last = ITERS - 1
    group = slots // col_count
    entries = [("image", i, j) for j in range(ITERS) for i in range(j + 1) if i < last]
    entries += [("source", 0, j) for j in range(ITERS)]
    groups = -(-len(entries) // group)

    def early_sums():
        pairs = []
        for kind, i, j in entries:
            left = images.at[i] if kind == "image" else source_ref
            pairs.append(dot(left, vectors.at[j]))
        filler = jnp.zeros((col_count, slots), jnp.float32)
        for at in range(groups):
            rows = pairs[at * group : (at + 1) * group]
            rows = rows + [(filler, filler)] * (group - len(rows))
            flat = [jnp.concatenate([pair[which] for pair in rows], axis=0).T for which in (0, 1)]
            slabs = [
                (flat[0][start : start + 8], flat[1][start : start + 8]) for start in range(0, slots, 8)
            ]
            pair = over_sublanes(tree(slabs, add), 8)
            gather_early[0, at : at + 1] = pair[0][0:1]
            gather_early[0, groups + at : groups + at + 1] = pair[1][0:1]

    for step in range(ITERS):
        if step == last:
            early_sums()
            start_all(*early_args)
        all_columns(store_product_part(step))
        end_halo(*vector_args(step))
        edge_columns(finish_product(step))
        if step < last:
            start_halo(LONG, *vector_args(step + 1))
        inner_columns(finish_product(step))
        if step < last:
            start_halo(SHORT, *vector_args(step + 1))
        set_image(step)

    pair = over_sublanes(dot(images.at[last], vectors.at[last]), col_count)
    flat = [jnp.broadcast_to(part_of[0:1], (slots, slots)).T for part_of in pair]
    slabs = [(flat[0][start : start + 8], flat[1][start : start + 8]) for start in range(0, slots, 8)]
    pair = over_sublanes(tree(slabs, add), 8)
    gather_late[0, 0:1] = pair[0][0:1]
    gather_late[0, 1:2] = pair[1][0:1]
    start_all(*late_args)

    end_all(*early_args)
    sums = {}
    for at in range(groups):
        pair = tree(
            [
                (gather_early[device, at : at + 1], gather_early[device, groups + at : groups + at + 1])
                for device in range(device_count)
            ],
            add,
        )
        flat = [spread(part_of) for part_of in pair]
        for index, entry in enumerate(entries[at * group : (at + 1) * group]):
            rows = slice(index * col_count, (index + 1) * col_count)
            sums[entry] = tidy(over_sublanes((flat[0][rows], flat[1][rows]), col_count))
    matrix = lambda i, j: sums["image", min(i, j), max(i, j)]

    zero = jnp.zeros((col_count, slots), jnp.float32)
    nothing = (zero, zero)
    unit = (zero + 1.0, zero)
    number = lambda value: (zero + value, zero)
    inverses, factors, directions, shares = [], {}, [], []
    kept_last = None
    for k in range(ITERS):
        scaled = {}
        for j in range(k):
            value = matrix(k, j)
            for i in range(j):
                value = sub(value, mul(scaled[i], factors[j, i]))
            scaled[j] = value
            factors[k, j] = mul(value, inverses[j])
        target = sums["source", 0, k]
        for j in range(k):
            target = sub(target, mul(factors[k, j], shares[j][0]))
        removed = nothing
        for j in range(k):
            removed = tidy(add(removed, mul(scaled[j], factors[k, j])))
        direction = [nothing] * k + [unit]
        for j in range(k):
            for i in range(j + 1):
                direction[i] = sub(direction[i], mul(factors[k, j], directions[j][i]))
        directions.append(direction)
        if k < last:
            pivot = sub(matrix(k, k), removed)
            inverses.append(inverse(pivot))
            shares.append((target, mul(target, inverses[k])))
        else:
            kept_last = (target, removed)

    def applied(direction):
        count = len(direction)
        padded = direction + [nothing, nothing]
        out = []
        for i in range(count + 1):
            value = mul(padded[i], number(1.0 - CENTRE))
            if i:
                value = sub(value, mul(padded[i - 1], number(HALF if i == 1 else HALF / 2)))
            out.append(sub(value, mul(padded[i + 1], number(HALF / 2))))
        return out

    def combined(coefficients, row):
        return tree([value[0] * vectors[i, row] for i, value in enumerate(coefficients)], jnp.add)

    solution = [nothing] * ITERS
    remainder = [unit] + [nothing] * ITERS
    peak_rows = []

    def largest(rows):
        peak = tree([jnp.abs(one) for one in rows], jnp.maximum)
        return jnp.max(jnp.max(peak, axis=0, keepdims=True), axis=1, keepdims=True)

    for k in range(last):
        share = shares[k][1]
        image = applied(directions[k])
        for i, value in enumerate(directions[k]):
            solution[i] = tidy(add(solution[i], mul(share, value)))
        for i, value in enumerate(image):
            remainder[i] = sub(remainder[i], mul(share, value))
        rows = [diag_ref[row] * combined(remainder[: k + 2], row) for row in range(row_count)]
        peak_rows.append(largest(rows))
    residual_rows = rows
    image = applied(directions[last])
    solution_rows = [combined(solution[:last], row) for row in range(row_count)]
    direction_rows = [combined(directions[last], row) for row in range(row_count)]
    image_rows = [diag_ref[row] * combined(image, row) for row in range(row_count)]

    end_all(*late_args)
    pair = tree(
        [(gather_late[device, 0:1], gather_late[device, 1:2]) for device in range(device_count)], add
    )
    target, removed = kept_last
    pivot = sub(tidy(pair), (removed[0][0:1], removed[1][0:1]))
    share = target[0][0:1] / pivot[0]
    for row in range(row_count):
        residual_rows[row] = residual_rows[row] - share * image_rows[row]
        residual_ref[row] = residual_rows[row]
        pressure_ref[row] = solution_rows[row] + share * direction_rows[row]
    peak_rows.append(largest(residual_rows))
    lane = lax.broadcasted_iota(jnp.int32, (1, slots), 1)
    packed = jnp.zeros((1, slots), jnp.float32)
    for k in range(ITERS):
        packed = jnp.where(lane == k, peak_rows[k], packed)
    gather_peak[0] = packed
    start_all(*peak_args)

    end_sends(*field_args)
    end_sends(*density_args)
    for step in range(ITERS):
        end_sends(*vector_args(step))
    end_all_sends(*early_args)
    end_all_sends(*late_args)
    end_all(*peak_args)
    peaks_ref[...] = tree([gather_peak[device] for device in range(device_count)], jnp.maximum)
    end_all_sends(*peak_args)


def write_out(density_ref, pressure_ref, residual_ref, peaks_ref, *rest):
    outs, sems = rest[:3], rest[4]
    rest[3][...] = peaks_ref[0, : rest[3].shape[0]]
    copies = [
        pltpu.make_async_copy(source, target, sems.at[index])
        for index, (source, target) in enumerate(zip((density_ref, pressure_ref, residual_ref), outs))
    ]
    for copy in copies:
        copy.start()
    for copy in copies:
        copy.wait()


def body(size_x, size_y, offsets, masses, counts, source):
    row_count, col_count, slots = masses.shape
    devices = size_x * size_y
    padded = (row_count + 2, col_count + 2)
    block = (row_count, col_count, slots)
    dma, f32, sides = pltpu.SemaphoreType.DMA, jnp.float32, len(SIDES)
    scratch = lambda *shape: pltpu.VMEM(shape, f32)
    early_rows = 2 * (-(-(ITERS * (ITERS + 1) // 2 - 1 + ITERS) // (slots // col_count)))
    vmem = pl.BlockSpec(memory_space=pltpu.VMEM)
    hbm = pl.BlockSpec(memory_space=pl.ANY)
    shaped = jax.ShapeDtypeStruct(block, f32)
    results = pl.pallas_call(
        functools.partial(kernel, size_x, size_y, row_count, col_count),
        out_shape=(shaped, shaped, shaped, jax.ShapeDtypeStruct((1, slots), f32)),
        in_specs=[hbm] * 4,
        out_specs=(vmem,) * 4,
        scratch_shapes=[
            scratch(2, *block), scratch(*block), pltpu.VMEM((row_count, col_count), jnp.int32),
            scratch(*block), dma((4,)),
            scratch(*padded, 4, slots), scratch(*padded, 1, slots), scratch(ITERS, *padded, 1, slots),
            scratch(row_count, col_count, len(NEIGHBOUR_STEPS), slots, slots),
            scratch(row_count, col_count, slots, slots),
            scratch(row_count, col_count, slots, slots),
            scratch(row_count, col_count, slots, slots),
            scratch(row_count, col_count, 1, slots),
            scratch(row_count, col_count, 1, slots),
            scratch(*block),
            scratch(ITERS + 1, *block), scratch(ITERS, *block), scratch(ITERS, *block),
            scratch(devices, early_rows, slots), scratch(devices, 2, slots), scratch(devices, 1, slots),
            dma((sides,)), dma((sides,)), dma((sides,)), dma((sides,)),
            dma((ITERS, sides)), dma((ITERS, sides)),
            dma((devices,)), dma((devices,)), dma((devices,)), dma((devices,)),
            dma((devices,)), dma((devices,)),
        ],
        compiler_params=pltpu.CompilerParams(collective_id=0, has_side_effects=True),
    )(offsets, masses, counts, source)
    return pl.pallas_call(
        write_out,
        out_shape=(shaped, shaped, shaped, jax.ShapeDtypeStruct((ITERS,), f32)),
        in_specs=[vmem] * 4,
        out_specs=(hbm, hbm, hbm, vmem),
        scratch_shapes=[dma((3,))],
    )(*results)


def solution(mesh):
    in_specs = (P(None, "gx", "gy", None), P("gx", "gy", None), P("gx", "gy"), P("gx", "gy", None))
    out_specs = (P("gx", "gy", None), P("gx", "gy", None), P("gx", "gy", None), P())
    return jax.shard_map(
        functools.partial(body, mesh.shape["gx"], mesh.shape["gy"]),
        mesh=mesh, in_specs=in_specs, out_specs=out_specs, check_vma=False,
    )
```

```python
import functools

import jax
import jax.numpy as jnp
from jax import lax
from jax.experimental import pallas as pl
from jax.experimental.pallas import tpu as pltpu
from jax.sharding import PartitionSpec as P

ITERS = 5
BASE_STIFF = 0.5
PAIR_SCALE = 0.05
NEIGHBOUR_STEPS = [(step_x, step_y) for step_x in (-1, 0, 1) for step_y in (-1, 0, 1)]
SIDES = [step for step in NEIGHBOUR_STEPS if step != (0, 0)]
MESH = pl.DeviceIdType.MESH
FAR = 64.0
CENTRE, HALF = 0.4375, 0.5
CHUNK = 64


def two_sum(a, b):
    total = a + b
    part = total - a
    return total, (a - (total - part)) + (b - part)


def add(a, b):
    high, low = two_sum(a[0], b[0])
    return high, low + (a[1] + b[1])


def tidy(a):
    high = a[0] + a[1]
    return high, a[1] - (high - a[0])


def halves(a):
    wide = a * 4097.0
    high = wide - (wide - a)
    return high, a - high


def mul(a, b):
    a_high, a_low = halves(a[0])
    b_high, b_low = halves(b[0])
    product = a[0] * b[0]
    rest = ((a_high * b_high - product) + (a_high * b_low + a_low * b_high)) + a_low * b_low
    return tidy((product, rest + (a[0] * b[1] + a[1] * b[0])))


def neg(a):
    return -a[0], -a[1]


def sub(a, b):
    return tidy(add(a, neg(b)))


def inverse(a):
    first = 1.0 / a[0]
    start = (first, jnp.zeros_like(first))
    one = (jnp.ones_like(first), jnp.zeros_like(first))
    rest = sub(one, mul(start, a))
    return tidy((first, rest[0] * first))


def tree(items, combine):
    items = list(items)
    while len(items) > 1:
        paired = [combine(items[at], items[at + 1]) for at in range(0, len(items) - 1, 2)]
        items = paired + items[len(paired) * 2 :]
    return items[0]


def over_sublanes(pair, rows):
    shift = rows // 2
    while shift:
        pair = add(pair, tuple(pltpu.roll(part, shift, 0) for part in pair))
        shift //= 2
    return pair


def kernel(
    size_x, size_y, row_count, col_count,
    offsets_hbm, masses_hbm, counts_hbm, source_hbm,
    density_ref, pressure_ref, residual_ref, peaks_ref,
    offsets_ref, masses_ref, counts_ref, source_ref, load_sem,
    pad_fields, pad_density, pad_vector, weights, own_x, own_y, own_density,
    part, inverse_diag, diag_ref, vectors, products, images,
    gather_early, gather_late, gather_peak,
    field_send, field_recv, density_send, density_recv, vector_send, vector_recv,
    early_send, early_recv, late_send, late_recv, peak_send, peak_recv,
):
    here_x, here_y = lax.axis_index("gx"), lax.axis_index("gy")
    device_count = size_x * size_y
    slots = masses_ref.shape[-1]

    loads = [
        pltpu.make_async_copy(source, target, load_sem.at[index])
        for index, (source, target) in enumerate((
            (offsets_hbm, offsets_ref), (masses_hbm, masses_ref),
            (counts_hbm, counts_ref), (source_hbm, source_ref),
        ))
    ]
    for load in loads:
        load.start()

    low_x, high_x = (here_x > 0), (here_x < size_x - 1)
    low_y, high_y = (here_y > 0), (here_y < size_y - 1)

    def on_side(step_x, step_y, action):
        conditions = []
        if step_x:
            conditions.append({1: high_x, -1: low_x}[step_x])
        if step_y:
            conditions.append({1: high_y, -1: low_y}[step_y])
        condition = conditions[0]
        for other in conditions[1:]:
            condition = jnp.logical_and(condition, other)
        pl.when(condition)(action)

    def ahead(here, step, size):
        there = here + step
        return jnp.where(there >= size, there - size, there)

    def for_peers(action):
        if device_count <= 64:
            for index in range(1, device_count):
                action(index, index // size_y, index % size_y)
        else:
            def one(index, carry):
                action(index, lax.div(index, size_y), lax.rem(index, size_y))
                return carry

            lax.fori_loop(1, device_count, one, 0)

    barrier = pltpu.get_barrier_semaphore()

    def greet(device):
        pl.semaphore_signal(barrier, inc=1, device_id=device, device_id_type=MESH)

    near_only = max(size_x, size_y) <= ITERS + 3
    if near_only:
        for step_x, step_y in SIDES:
            on_side(step_x, step_y, functools.partial(greet, (here_x + step_x, here_y + step_y)))
    else:
        for_peers(lambda index, step_x, step_y: greet(
            (ahead(here_x, step_x, size_x), ahead(here_y, step_y, size_y))
        ))

    def fill(ref, value):
        ref[...] = jnp.full(ref.shape, value, jnp.float32)

    def fill_outside(at):
        fill(pad_fields.at[at], FAR)
        fill(pad_density.at[at], 0.0)
        for step in range(ITERS):
            fill(pad_vector.at[(step,) + at], 0.0)

    every = slice(None)
    pl.when(jnp.logical_not(low_x))(lambda: fill_outside((0, every)))
    pl.when(jnp.logical_not(high_x))(lambda: fill_outside((row_count + 1, every)))
    pl.when(jnp.logical_not(low_y))(lambda: fill_outside((every, 0)))
    pl.when(jnp.logical_not(high_y))(lambda: fill_outside((every, col_count + 1)))

    def halo_copy(side, pad, send_sem, recv_sem):
        step_x, step_y = SIDES[side]
        inner = lambda step, count: {1: pl.ds(count, 1), -1: pl.ds(1, 1), 0: pl.ds(1, count)}[step]
        outer = lambda step, count: {1: pl.ds(0, 1), -1: pl.ds(count + 1, 1), 0: pl.ds(1, count)}[step]
        return pltpu.make_async_remote_copy(
            src_ref=pad.at[inner(step_x, row_count), inner(step_y, col_count)],
            dst_ref=pad.at[outer(step_x, row_count), outer(step_y, col_count)],
            send_sem=send_sem.at[side],
            recv_sem=recv_sem.at[side],
            device_id=(here_x + step_x, here_y + step_y),
            device_id_type=MESH,
        )

    LONG = [side for side, step in enumerate(SIDES) if step[1]]
    SHORT = [side for side, step in enumerate(SIDES) if not step[1]]

    def start_halo(sides, *args):
        for side in sides:
            on_side(*SIDES[side], lambda side=side: halo_copy(side, *args).start())

    def end_halo(*args):
        for side, (step_x, step_y) in enumerate(SIDES):
            on_side(-step_x, -step_y, lambda side=side: halo_copy(side, *args).wait_recv())

    def end_sends(*args):
        for side, (step_x, step_y) in enumerate(SIDES):
            on_side(step_x, step_y, lambda side=side: halo_copy(side, *args).wait_send())

    def steps_of(row, place, inside):
        def is_inside(step_x, step_y):
            if not 0 <= row + step_x < row_count:
                return False
            return not (place == "first" and step_y < 0 or place == "last" and step_y > 0)

        return [
            (index, step_x, step_y)
            for index, (step_x, step_y) in enumerate(NEIGHBOUR_STEPS)
            if is_inside(step_x, step_y) == inside
        ]

    def edge_columns(action):
        for col, place in ((0, "first"), (col_count - 1, "last")):
            for row in range(row_count):
                action(row, col, place)

    def inner_columns(action, unroll=True):
        def one(col, carry):
            for row in range(row_count):
                action(row, col, "inner")
            return carry

        if unroll:
            for col in range(1, col_count - 1):
                one(col, 0)
        else:
            lax.fori_loop(1, col_count - 1, one, 0)

    def all_columns(action, unroll=True):
        edge_columns(action)
        inner_columns(action, unroll)

    def spread(row):
        return jnp.broadcast_to(row, (slots, slots)).T

    def gathered(total):
        return jnp.sum(total.T, axis=0, keepdims=True)

    def chunks(terms):
        return gathered(jnp.concatenate(
            [terms(pl.ds(start, CHUNK)) for start in range(0, slots, CHUNK)], axis=0
        ))

    for load in loads:
        load.wait()
    lane = lax.broadcasted_iota(jnp.int32, (col_count, slots), 1)
    square = (col_count, col_count)
    on_diagonal = lax.broadcasted_iota(jnp.int32, square, 0) == lax.broadcasted_iota(jnp.int32, square, 1)
    occupied = []
    for row in range(row_count):
        limits = jnp.where(
            on_diagonal, jnp.broadcast_to(counts_ref[row : row + 1].astype(jnp.float32), square), 0.0
        )
        limit = jnp.sum(limits, axis=1, keepdims=True)
        occupied.append((lane.astype(jnp.float32) < limit).astype(jnp.float32))
        live = occupied[row] > 0.0
        field_rows = (
            jnp.where(live, offsets_ref[0, row], FAR),
            jnp.where(live, offsets_ref[1, row], FAR),
            masses_ref[row],
            source_ref[row] * occupied[row],
        )
        source_ref[row] = field_rows[3]
        for col in range(col_count):
            for index in range(3):
                pad_fields[row + 1, col + 1, index : index + 1] = field_rows[index][col : col + 1]
        inverse_diag[row] = occupied[row].reshape(col_count, 1, slots)

    greeters = lambda low, high: low.astype(jnp.int32) + high.astype(jnp.int32)
    if near_only:
        count_x, count_y = greeters(low_x, high_x), greeters(low_y, high_y)
        pl.semaphore_wait(barrier, (count_x + 1) * (count_y + 1) - 1)
    else:
        pl.semaphore_wait(barrier, device_count - 1)

    field_args = (pad_fields, field_send, field_recv)
    start_halo(range(len(SIDES)), *field_args)

    def spread_place(row, col, place):
        own_x[row, col] = spread(offsets_ref[0, row, pl.ds(col, 1)])
        own_y[row, col] = spread(offsets_ref[1, row, pl.ds(col, 1)])

    all_columns(spread_place)

    def density_part(inside):
        def one(row, col, place):
            steps = steps_of(row, place, inside)

            def terms(rows):
                at_x, at_y = own_x[row, col, rows], own_y[row, col, rows]
                total = None
                for index, step_x, step_y in steps:
                    near = pad_fields[row + 1 + step_x, col + 1 + step_y]
                    offset_x = (step_x + near[0:1]) - at_x
                    offset_y = (step_y + near[1:2]) - at_y
                    falloff = jnp.maximum(1.0 - (offset_x * offset_x + offset_y * offset_y), 0.0)
                    squared = falloff * falloff
                    weights[row, col, index, rows] = squared
                    term = squared * falloff * near[2:3]
                    total = term if total is None else total + term
                return total

            return chunks(terms)

        return one

    def store_density_part(row, col, place):
        part[row, col] = density_part(True)(row, col, place)

    all_columns(store_density_part)
    end_halo(*field_args)

    def finish_density(row, col, place):
        density = 1.0 + (part[row, col] + density_part(False)(row, col, place))
        pad_density[row + 1, col + 1] = density
        density_ref[row, pl.ds(col, 1)] = density

    density_args = (pad_density, density_send, density_recv)
    edge_columns(finish_density)
    start_halo(LONG, *density_args)
    inner_columns(finish_density)
    start_halo(SHORT, *density_args)

    def weight_part(inside):
        def one(row, col, place):
            steps = steps_of(row, place, inside)

            def terms(rows):
                here = own_density[row, col, rows]
                total = None
                for index, step_x, step_y in steps:
                    there = pad_density[row + 1 + step_x, col + 1 + step_y]
                    weight = weights[row, col, index, rows] * ((2.0 * PAIR_SCALE) / (here + there))
                    weights[row, col, index, rows] = weight
                    total = weight if total is None else total + weight
                return total

            return chunks(terms)

        return one

    def store_weight_part(row, col, place):
        own_density[row, col] = spread(pad_density[row + 1, col + 1])
        part[row, col] = weight_part(True)(row, col, place)

    all_columns(store_weight_part)
    end_halo(*density_args)

    def finish_weights(row, col, place):
        occupied_row = inverse_diag[row, col]
        total = part[row, col] + weight_part(False)(row, col, place)
        diagonal = BASE_STIFF + occupied_row * total
        inverted = occupied_row / diagonal
        scaled = source_ref[row, pl.ds(col, 1)] * inverted
        diag_ref[row, pl.ds(col, 1)] = diagonal
        inverse_diag[row, col] = inverted
        vectors[0, row, pl.ds(col, 1)] = scaled
        pad_vector[0, row + 1, col + 1] = scaled

    def vector_args(step):
        return pad_vector.at[step], vector_send.at[step], vector_recv.at[step]

    edge_columns(finish_weights)
    start_halo(LONG, *vector_args(0))
    inner_columns(finish_weights)
    start_halo(SHORT, *vector_args(0))

    def product_part(step, inside):
        def one(row, col, place):
            total = None
            for index, step_x, step_y in steps_of(row, place, inside):
                term = weights[row, col, index] * pad_vector[step, row + 1 + step_x, col + 1 + step_y]
                total = term if total is None else total + term
            return gathered(total)

        return one

    def store_product_part(step):
        def one(row, col, place):
            part[row, col] = product_part(step, True)(row, col, place)

        return one

    def finish_product(step):
        def one(row, col, place):
            product = part[row, col] + product_part(step, False)(row, col, place)
            products[step, row, pl.ds(col, 1)] = product
            now = vectors[step, row, pl.ds(col, 1)]
            rest = inverse_diag[row, col] * product - CENTRE * now
            if step == 0:
                following = rest * (1.0 / HALF)
            else:
                following = rest * (2.0 / HALF) - vectors[step - 1, row, pl.ds(col, 1)]
            vectors[step + 1, row, pl.ds(col, 1)] = following
            if step + 1 < ITERS:
                pad_vector[step + 1, row + 1, col + 1] = following

        return one

    def set_image(step):
        for row in range(row_count):
            images[step, row] = diag_ref[row] * vectors[step, row] - products[step, row]

    def dot(left, right):
        zero = jnp.zeros((col_count, slots), jnp.float32)
        return tree([(left[row] * right[row], zero) for row in range(row_count)], add)

    def send_all(gather, send_sem, recv_sem):
        def one(index, step_x, step_y):
            return pltpu.make_async_remote_copy(
                src_ref=gather.at[0],
                dst_ref=gather.at[index],
                send_sem=send_sem.at[index],
                recv_sem=recv_sem.at[index],
                device_id=(ahead(here_x, step_x, size_x), ahead(here_y, step_y, size_y)),
                device_id_type=MESH,
            )

        return one

    def start_all(*args):
        for_peers(lambda *peer: send_all(*args)(*peer).start())

    def end_all(*args):
        for_peers(lambda *peer: send_all(*args)(*peer).wait_recv())

    def end_all_sends(*args):
        for_peers(lambda *peer: send_all(*args)(*peer).wait_send())

    early_args = (gather_early, early_send, early_recv)
    late_args = (gather_late, late_send, late_recv)
    peak_args = (gather_peak, peak_send, peak_recv)
    last = ITERS - 1
    group = slots // col_count
    entries = [("image", i, j) for j in range(ITERS) for i in range(j + 1) if i < last]
    entries += [("source", 0, j) for j in range(ITERS)]
    groups = -(-len(entries) // group)

    def early_sums():
        pairs = []
        for kind, i, j in entries:
            left = images.at[i] if kind == "image" else source_ref
            pairs.append(dot(left, vectors.at[j]))
        filler = jnp.zeros((col_count, slots), jnp.float32)
        for at in range(groups):
            rows = pairs[at * group : (at + 1) * group]
            rows = rows + [(filler, filler)] * (group - len(rows))
            flat = [jnp.concatenate([pair[which] for pair in rows], axis=0).T for which in (0, 1)]
            slabs = [
                (flat[0][start : start + 8], flat[1][start : start + 8]) for start in range(0, slots, 8)
            ]
            pair = over_sublanes(tree(slabs, add), 8)
            gather_early[0, at : at + 1] = pair[0][0:1]
            gather_early[0, groups + at : groups + at + 1] = pair[1][0:1]

    def sum_lanes(pair):
        flat = [jnp.broadcast_to(part_of[0:1], (slots, slots)).T for part_of in pair]
        slabs = [(flat[0][start : start + 8], flat[1][start : start + 8]) for start in range(0, slots, 8)]
        return over_sublanes(tree(slabs, add), 8)

    def end_product(step):
        edge_columns(finish_product(step))
        if step < last:
            start_halo(LONG, *vector_args(step + 1))
        inner_columns(finish_product(step))
        if step < last:
            start_halo(SHORT, *vector_args(step + 1))
            set_image(step)

    for step in range(last):
        all_columns(store_product_part(step))
        end_halo(*vector_args(step))
        end_product(step)
    early_sums()
    start_all(*early_args)
    all_columns(store_product_part(last))

    for row in range(row_count):
        for col in range(col_count):
            own_x[row, col] = spread(vectors[last, row, pl.ds(col, 1)])
            products[last, row, pl.ds(col, 1)] = part[row, col]
    set_image(last)
    inside_sum = dot(images.at[last], vectors.at[last])
    end_halo(*vector_args(last))
    crossing = []
    for row in range(row_count):
        for col in range(col_count):
            place = "first" if col == 0 else "last" if col == col_count - 1 else "inner"
            total = None
            for index, step_x, step_y in steps_of(row, place, False):
                term = weights[row, col, index] * pad_vector[last, row + 1 + step_x, col + 1 + step_y]
                total = term if total is None else total + term
            total = total * own_x[row, col]
            crossing.append(tree([total[start : start + 8] for start in range(0, slots, 8)], jnp.add))
    zero = jnp.zeros((8, slots), jnp.float32)
    crossing = tree([(-one, zero) for one in crossing], add)
    pair = over_sublanes(add(inside_sum, crossing), 8)
    pair = sum_lanes(pair)
    gather_late[0, 0:1] = pair[0][0:1]
    gather_late[0, 1:2] = pair[1][0:1]
    start_all(*late_args)

    end_product(last)
    end_all(*early_args)
    sums = {}
    for at in range(groups):
        pair = tree(
            [
                (gather_early[device, at : at + 1], gather_early[device, groups + at : groups + at + 1])
                for device in range(device_count)
            ],
            add,
        )
        flat = [spread(part_of) for part_of in pair]
        for index, entry in enumerate(entries[at * group : (at + 1) * group]):
            rows = slice(index * col_count, (index + 1) * col_count)
            sums[entry] = tidy(over_sublanes((flat[0][rows], flat[1][rows]), col_count))
    matrix = lambda i, j: sums["image", min(i, j), max(i, j)]

    zero = jnp.zeros((col_count, slots), jnp.float32)
    nothing = (zero, zero)
    unit = (zero + 1.0, zero)
    number = lambda value: (zero + value, zero)
    inverses, factors, directions, shares = [], {}, [], []
    kept_last = None
    for k in range(ITERS):
        scaled = {}
        for j in range(k):
            value = matrix(k, j)
            for i in range(j):
                value = sub(value, mul(scaled[i], factors[j, i]))
            scaled[j] = value
            factors[k, j] = mul(value, inverses[j])
        target = sums["source", 0, k]
        for j in range(k):
            target = sub(target, mul(factors[k, j], shares[j][0]))
        removed = nothing
        for j in range(k):
            removed = tidy(add(removed, mul(scaled[j], factors[k, j])))
        direction = [nothing] * k + [unit]
        for j in range(k):
            for i in range(j + 1):
                direction[i] = sub(direction[i], mul(factors[k, j], directions[j][i]))
        directions.append(direction)
        if k < last:
            pivot = sub(matrix(k, k), removed)
            inverses.append(inverse(pivot))
            shares.append((target, mul(target, inverses[k])))
        else:
            kept_last = (target, removed)

    def applied(direction):
        count = len(direction)
        padded = direction + [nothing, nothing]
        out = []
        for i in range(count + 1):
            value = mul(padded[i], number(1.0 - CENTRE))
            if i:
                value = sub(value, mul(padded[i - 1], number(HALF if i == 1 else HALF / 2)))
            out.append(sub(value, mul(padded[i + 1], number(HALF / 2))))
        return out

    def combined(coefficients, row):
        return tree([value[0] * vectors[i, row] for i, value in enumerate(coefficients)], jnp.add)

    solution = [nothing] * ITERS
    remainder = [unit] + [nothing] * ITERS
    peak_rows = []

    def largest(rows):
        peak = tree([jnp.abs(one) for one in rows], jnp.maximum)
        return jnp.max(jnp.max(peak, axis=0, keepdims=True), axis=1, keepdims=True)

    for k in range(last):
        share = shares[k][1]
        image = applied(directions[k])
        for i, value in enumerate(directions[k]):
            solution[i] = tidy(add(solution[i], mul(share, value)))
        for i, value in enumerate(image):
            remainder[i] = sub(remainder[i], mul(share, value))
        rows = [diag_ref[row] * combined(remainder[: k + 2], row) for row in range(row_count)]
        peak_rows.append(largest(rows))
    residual_rows = rows
    image = applied(directions[last])
    solution_rows = [combined(solution[:last], row) for row in range(row_count)]
    direction_rows = [combined(directions[last], row) for row in range(row_count)]
    image_rows = [diag_ref[row] * combined(image, row) for row in range(row_count)]

    end_all(*late_args)
    pair = tree(
        [(gather_late[device, 0:1], gather_late[device, 1:2]) for device in range(device_count)], add
    )
    target, removed = kept_last
    pivot = sub(tidy(pair), (removed[0][0:1], removed[1][0:1]))
    share = target[0][0:1] / pivot[0]
    for row in range(row_count):
        residual_rows[row] = residual_rows[row] - share * image_rows[row]
        residual_ref[row] = residual_rows[row]
        pressure_ref[row] = solution_rows[row] + share * direction_rows[row]
    peak_rows.append(largest(residual_rows))
    lane = lax.broadcasted_iota(jnp.int32, (1, slots), 1)
    packed = jnp.zeros((1, slots), jnp.float32)
    for k in range(ITERS):
        packed = jnp.where(lane == k, peak_rows[k], packed)
    gather_peak[0] = packed
    start_all(*peak_args)

    end_sends(*field_args)
    end_sends(*density_args)
    for step in range(ITERS):
        end_sends(*vector_args(step))
    end_all_sends(*early_args)
    end_all_sends(*late_args)
    end_all(*peak_args)
    peaks_ref[...] = tree([gather_peak[device] for device in range(device_count)], jnp.maximum)
    end_all_sends(*peak_args)


def write_out(density_ref, pressure_ref, residual_ref, peaks_ref, *rest):
    outs, packed_ref, sems = rest[:4], rest[4], rest[5]
    packed_ref[...] = peaks_ref[0, : packed_ref.shape[0]]
    copies = [
        pltpu.make_async_copy(source, target, sems.at[index])
        for index, (source, target) in enumerate(
            zip((density_ref, pressure_ref, residual_ref, packed_ref), outs)
        )
    ]
    for copy in copies:
        copy.start()
    for copy in copies:
        copy.wait()


def body(size_x, size_y, offsets, masses, counts, source):
    row_count, col_count, slots = masses.shape
    devices = size_x * size_y
    padded = (row_count + 2, col_count + 2)
    block = (row_count, col_count, slots)
    dma, f32, sides = pltpu.SemaphoreType.DMA, jnp.float32, len(SIDES)
    scratch = lambda *shape: pltpu.VMEM(shape, f32)
    early_rows = 2 * (-(-(ITERS * (ITERS + 1) // 2 - 1 + ITERS) // (slots // col_count)))
    weight_bytes = 4 * row_count * col_count * len(NEIGHBOUR_STEPS) * slots * slots
    vmem = pl.BlockSpec(memory_space=pltpu.VMEM)
    hbm = pl.BlockSpec(memory_space=pltpu.HBM)
    shaped = jax.ShapeDtypeStruct(block, f32)
    results = pl.pallas_call(
        functools.partial(kernel, size_x, size_y, row_count, col_count),
        out_shape=(shaped, shaped, shaped, jax.ShapeDtypeStruct((1, slots), f32)),
        in_specs=[hbm] * 4,
        out_specs=(vmem,) * 4,
        scratch_shapes=[
            scratch(2, *block), scratch(*block), pltpu.VMEM((row_count, col_count), jnp.int32),
            scratch(*block), dma((4,)),
            scratch(*padded, 4, slots), scratch(*padded, 1, slots), scratch(ITERS, *padded, 1, slots),
            scratch(row_count, col_count, len(NEIGHBOUR_STEPS), slots, slots),
            scratch(row_count, col_count, slots, slots),
            scratch(row_count, col_count, slots, slots),
            scratch(row_count, col_count, slots, slots),
            scratch(row_count, col_count, 1, slots),
            scratch(row_count, col_count, 1, slots),
            scratch(*block),
            scratch(ITERS + 1, *block), scratch(ITERS, *block), scratch(ITERS, *block),
            scratch(devices, early_rows, slots), scratch(devices, 2, slots), scratch(devices, 1, slots),
            dma((sides,)), dma((sides,)), dma((sides,)), dma((sides,)),
            dma((ITERS, sides)), dma((ITERS, sides)),
            dma((devices,)), dma((devices,)), dma((devices,)), dma((devices,)),
            dma((devices,)), dma((devices,)),
        ],
        compiler_params=pltpu.CompilerParams(
            collective_id=0, has_side_effects=True, vmem_limit_bytes=3 * weight_bytes
        ),
    )(*(pltpu.with_memory_space_constraint(one, pltpu.HBM) for one in (offsets, masses, counts, source)))
    return pl.pallas_call(
        write_out,
        out_shape=(shaped, shaped, shaped, jax.ShapeDtypeStruct((ITERS,), f32)),
        in_specs=[vmem] * 4,
        out_specs=(hbm,) * 4,
        scratch_shapes=[scratch(ITERS), dma((4,))],
        compiler_params=pltpu.CompilerParams(vmem_limit_bytes=weight_bytes),
    )(*results)


def solution(mesh):
    in_specs = (P(None, "gx", "gy", None), P("gx", "gy", None), P("gx", "gy"), P("gx", "gy", None))
    out_specs = (P("gx", "gy", None), P("gx", "gy", None), P("gx", "gy", None), P())
    return jax.shard_map(
        functools.partial(body, mesh.shape["gx"], mesh.shape["gy"]),
        mesh=mesh, in_specs=in_specs, out_specs=out_specs, check_vma=False,
    )
```

```python
import functools

import jax
import jax.numpy as jnp
from jax import lax
from jax.experimental import pallas as pl
from jax.experimental.pallas import tpu as pltpu
from jax.sharding import PartitionSpec as P

ITERS = 5
BASE_STIFF = 0.5
PAIR_SCALE = 0.05
NEIGHBOUR_STEPS = [(step_x, step_y) for step_x in (-1, 0, 1) for step_y in (-1, 0, 1)]
SIDES = [step for step in NEIGHBOUR_STEPS if step != (0, 0)]
MESH = pl.DeviceIdType.MESH
FAR = 64.0
CENTRE, HALF = 0.4375, 0.5
CHUNK = 64
DEEP = (1, 3)
READY = 9
FIRST = 13
MIDDLE = 0.5


def two_sum(a, b):
    total = a + b
    part = total - a
    return total, (a - (total - part)) + (b - part)


def add(a, b):
    high, low = two_sum(a[0], b[0])
    return high, low + (a[1] + b[1])


def tidy(a):
    high = a[0] + a[1]
    return high, a[1] - (high - a[0])


def halves(a):
    wide = a * 4097.0
    high = wide - (wide - a)
    return high, a - high


def mul(a, b):
    a_high, a_low = halves(a[0])
    b_high, b_low = halves(b[0])
    product = a[0] * b[0]
    rest = ((a_high * b_high - product) + (a_high * b_low + a_low * b_high)) + a_low * b_low
    return tidy((product, rest + (a[0] * b[1] + a[1] * b[0])))


def neg(a):
    return -a[0], -a[1]


def sub(a, b):
    return tidy(add(a, neg(b)))


def inverse(a):
    first = 1.0 / a[0]
    start = (first, jnp.zeros_like(first))
    one = (jnp.ones_like(first), jnp.zeros_like(first))
    rest = sub(one, mul(start, a))
    return tidy((first, rest[0] * first))


def tree(items, combine):
    items = list(items)
    while len(items) > 1:
        paired = [combine(items[at], items[at + 1]) for at in range(0, len(items) - 1, 2)]
        items = paired + items[len(paired) * 2 :]
    return items[0]


def over_sublanes(pair, rows):
    shift = rows // 2
    while shift:
        pair = add(pair, tuple(pltpu.roll(part, shift, 0) for part in pair))
        shift //= 2
    return pair


def kernel(
    size_x, size_y, row_count, col_count,
    offsets_hbm, masses_hbm, counts_hbm, source_hbm,
    density_ref, pressure_ref, residual_ref, peaks_ref,
    offsets_ref, masses_ref, counts_ref, source_ref, load_sem,
    pad_fields, pad_density, pad_vector, weights, own_x, own_y, own_density,
    part, inverse_diag, diag_ref, vectors, products, images,
    deep_places, deep_density, ring_weights, ring_inverse, ring_part, ring_own,
    gather_early, gather_late, gather_peak,
    field_send, field_recv, density_send, density_recv, vector_send, vector_recv,
    early_send, early_recv, late_send, late_recv, peak_send, peak_recv,
    deep_places_send, deep_places_recv, deep_density_send, deep_density_recv,
):
    here_x, here_y = lax.axis_index("gx"), lax.axis_index("gy")
    device_count = size_x * size_y
    slots = masses_ref.shape[-1]

    loads = [
        pltpu.make_async_copy(source, target, load_sem.at[index])
        for index, (source, target) in enumerate((
            (offsets_hbm, offsets_ref), (masses_hbm, masses_ref),
            (counts_hbm, counts_ref), (source_hbm, source_ref),
        ))
    ]
    for load in loads:
        load.start()

    low_x, high_x = (here_x > 0), (here_x < size_x - 1)
    low_y, high_y = (here_y > 0), (here_y < size_y - 1)

    def on_side(step_x, step_y, action):
        conditions = []
        if step_x:
            conditions.append({1: high_x, -1: low_x}[step_x])
        if step_y:
            conditions.append({1: high_y, -1: low_y}[step_y])
        condition = conditions[0]
        for other in conditions[1:]:
            condition = jnp.logical_and(condition, other)
        pl.when(condition)(action)

    def ahead(here, step, size):
        there = here + step
        return jnp.where(there >= size, there - size, there)

    def for_peers(action):
        def turned(step_y):
            return jnp.where(here_y < size_y // 2, size_y - step_y, step_y)

        if device_count <= 64:
            for step_y in range(1, size_y):
                for step_x in range(size_x - 1, -1, -1):
                    action(step_x * size_y + turned(step_y), step_x, turned(step_y))
            for step_x in range(1, size_x):
                action(step_x * size_y, step_x, 0)
        else:
            def one(index, carry):
                action(index, lax.div(index, size_y), lax.rem(index, size_y))
                return carry

            lax.fori_loop(1, device_count, one, 0)

    barrier = pltpu.get_barrier_semaphore()

    def greet(device):
        pl.semaphore_signal(barrier, inc=1, device_id=device, device_id_type=MESH)

    near_only = size_x <= ITERS + 2 and size_y <= ITERS + 3
    if near_only:
        for step_x, step_y in SIDES:
            on_side(step_x, step_y, functools.partial(greet, (here_x + step_x, here_y + step_y)))
        pl.when(here_y > 1)(lambda: greet((here_x, here_y - 2)))
        pl.when(here_y < size_y - 2)(lambda: greet((here_x, here_y + 2)))
    else:
        for_peers(lambda index, step_x, step_y: greet(
            (ahead(here_x, step_x, size_x), ahead(here_y, step_y, size_y))
        ))

    def fill(ref, value):
        ref[...] = jnp.full(ref.shape, value, jnp.float32)

    def fill_outside(axis, start):
        def at(margin):
            span = pl.ds(start + margin if start > 0 else 0, margin)
            return (span, slice(None)) if axis == 0 else (slice(None), span)

        fill(pad_fields.at[at(1)], FAR)
        fill(pad_density.at[at(1)], 1.0)
        fill(deep_places.at[at(2)], FAR)
        fill(deep_density.at[at(2)], 1.0)
        for step in range(ITERS):
            fill(pad_vector.at[(step,) + at(2)], 0.0)

    pl.when(jnp.logical_not(low_x))(lambda: fill_outside(0, 0))
    pl.when(jnp.logical_not(high_x))(lambda: fill_outside(0, row_count))
    pl.when(jnp.logical_not(low_y))(lambda: fill_outside(1, 0))
    pl.when(jnp.logical_not(high_y))(lambda: fill_outside(1, col_count))

    def halo_copy(side, pad, depth, send_sem, recv_sem):
        step_x, step_y = SIDES[side]
        margin = (pad.shape[0] - row_count) // 2

        def inner(step, count):
            start = margin + count - depth if step > 0 else margin
            return pl.ds(start, depth if step else count)

        def outer(step, count):
            start = {1: margin - depth, -1: margin + count, 0: margin}[step]
            return pl.ds(start, depth if step else count)

        return pltpu.make_async_remote_copy(
            src_ref=pad.at[inner(step_x, row_count), inner(step_y, col_count)],
            dst_ref=pad.at[outer(step_x, row_count), outer(step_y, col_count)],
            send_sem=send_sem.at[side],
            recv_sem=recv_sem.at[side],
            device_id=(here_x + step_x, here_y + step_y),
            device_id_type=MESH,
        )

    LONG = [side for side, step in enumerate(SIDES) if step[1]]
    SHORT = [side for side, step in enumerate(SIDES) if not step[1]]

    def start_halo(sides, *args):
        for side in sides:
            on_side(*SIDES[side], lambda side=side: halo_copy(side, *args).start())

    def end_halo(*args):
        for side, (step_x, step_y) in enumerate(SIDES):
            on_side(-step_x, -step_y, lambda side=side: halo_copy(side, *args).wait_recv())

    def end_sends(*args):
        for side, (step_x, step_y) in enumerate(SIDES):
            on_side(step_x, step_y, lambda side=side: halo_copy(side, *args).wait_send())

    def steps_of(row, place, inside):
        def is_inside(step_x, step_y):
            if not 0 <= row + step_x < row_count:
                return False
            return not (place == "first" and step_y < 0 or place == "last" and step_y > 0)

        return [
            (index, step_x, step_y)
            for index, (step_x, step_y) in enumerate(NEIGHBOUR_STEPS)
            if inside is None or is_inside(step_x, step_y) == inside
        ]

    def columns(action, chosen):
        for col in chosen:
            place = "first" if col == 0 else "last" if col == col_count - 1 else "inner"
            for row in range(row_count):
                action(row, col, place)

    def edge_columns(action, depth=1):
        columns(action, [col for col in range(col_count) if not depth <= col < col_count - depth])

    def inner_columns(action, depth=1):
        columns(action, range(depth, col_count - depth))

    def all_columns(action):
        edge_columns(action)
        inner_columns(action)

    def spread(row):
        return jnp.broadcast_to(row, (slots, slots)).T

    def gathered(total):
        return jnp.sum(total.T, axis=0, keepdims=True)

    def chunks(terms):
        return gathered(jnp.concatenate(
            [terms(pl.ds(start, CHUNK)) for start in range(0, slots, CHUNK)], axis=0
        ))

    wide = col_count + 2
    ring = [(col + 1, -1, col) for col in range(-1, col_count + 1)]
    ring += [(wide + col + 1, row_count, col) for col in range(-1, col_count + 1)]
    ring += [(2 * wide + 2 * row, row, -1) for row in range(row_count)]
    ring += [(2 * wide + 2 * row + 1, row, col_count) for row in range(row_count)]

    ring_middle = [cell for cell in ring if 3 <= cell[2] < col_count - 3]
    ring_ends = [cell for cell in ring if cell not in ring_middle]
    ring_at = {(row, col): at for at, row, col in ring}

    def known(at, row, col):
        out = []
        for index, (step_x, step_y) in enumerate(NEIGHBOUR_STEPS):
            cell = (row + step_x, col + step_y)
            back = len(NEIGHBOUR_STEPS) - 1 - index
            if 0 <= cell[0] < row_count and 0 <= cell[1] < col_count:
                out.append(("own", cell, back))
            elif cell in ring_at and order[ring_at[cell]] < order[at]:
                out.append(("ring", ring_at[cell], back))
            else:
                out.append(None)
        return out

    order = {at: place for place, (at, _, _) in enumerate(ring)}

    def spread_ring_places(at, row, col):
        places = deep_places[row + 2, col + 2]
        ring_own[at, 0] = spread(2.0 * places[0:1])
        ring_own[at, 1] = spread(2.0 * places[1:2])

    def spread_ring(at, row, col):
        if order[at] >= READY:
            spread_ring_places(at, row, col)
        ring_own[at, 2] = spread(deep_density[row + 2, col + 2])

    def in_turn(prepare, action, cells):
        prepare(*cells[0])
        for place, cell in enumerate(cells):
            if place + 1 < len(cells):
                prepare(*cells[place + 1])
            action(*cell)

    def ring_squares(at, row, col, rows):
        twice_x, twice_y = ring_own[at, 0, rows], ring_own[at, 1, rows]
        rest = 1.0 - 0.25 * (twice_x * twice_x + twice_y * twice_y)

        def one(index):
            step_x, step_y = NEIGHBOUR_STEPS[index]
            near = deep_places[row + 2 + step_x, col + 2 + step_y]
            near_x, near_y = near[0:1] + step_x, near[1:2] + step_y
            near_rest = near_x * near_x + near_y * near_y
            falloff = (rest - near_rest) + (twice_x * near_x + twice_y * near_y)
            falloff = jnp.maximum(falloff, 0.0)
            return falloff * falloff

        return one

    def parts():
        return [slice(start, start + CHUNK) for start in range(0, slots, CHUNK)]

    def set_ring_squares(at, row, col):
        for rows in parts():
            squares = ring_squares(at, row, col, rows)
            for index, found in enumerate(known(at, row, col)):
                if found is None:
                    ring_weights[at, index, rows] = squares(index)

    def set_ring_weights(at, row, col):
        ready = order[at] < READY
        totals = []
        turned = {}
        for index, found in enumerate(known(at, row, col)):
            if found is None:
                continue
            kind, cell, back = found
            if kind == "own":
                turned[index] = weights[cell[0], cell[1], back].T
                places = deep_places[cell[0] + 2, cell[1] + 2]
                live = (places[0:1] < FAR / 2).astype(jnp.float32)
            else:
                turned[index] = ring_weights[cell, back].T
                live = 1.0
            ring_weights[at, index] = turned[index]
            turned[index] = turned[index] * live
        for rows in parts():
            squares = None if ready else ring_squares(at, row, col, rows)
            here = ring_own[at, 2, rows]
            total = None
            for index, (step_x, step_y) in enumerate(NEIGHBOUR_STEPS):
                if index in turned:
                    weight = turned[index][rows]
                else:
                    there = deep_density[row + 2 + step_x, col + 2 + step_y]
                    square = ring_weights[at, index, rows] if ready else squares(index)
                    weight = square / (here + there)
                    ring_weights[at, index, rows] = weight
                total = weight if total is None else total + weight
            totals.append(total)
        total = gathered(jnp.concatenate(totals, axis=0))
        live = (deep_places[row + 2, col + 2][0:1] < FAR / 2).astype(jnp.float32)
        ring_inverse[at] = live / (BASE_STIFF + live * total)

    def set_ring_share(step):
        if step > DEEP[0]:
            return
        if step == 0:
            end_halo(*deep_density_args)
        share = ring[:FIRST] if step == 0 else ring[FIRST:]
        in_turn(spread_ring, set_ring_weights, share)

    def ring_product(step, at, row, col, inside):
        total = None
        for index, (step_x, step_y) in enumerate(NEIGHBOUR_STEPS):
            own = 0 <= row + step_x < row_count and 0 <= col + step_y < col_count
            if inside is None or own == inside:
                term = ring_weights[at, index] * pad_vector[step, row + 2 + step_x, col + 2 + step_y]
                total = term if total is None else total + term
        return gathered(total)

    def start_ring(step):
        if step == DEEP[1]:
            for at, row, col in ring:
                ring_part[at] = ring_product(step, at, row, col, True)

    def finish_ring(step, cells):
        for at, row, col in cells:
            if step == DEEP[1]:
                product = ring_part[at] + ring_product(step, at, row, col, False)
            else:
                product = ring_product(step, at, row, col, None)
            rest = ring_inverse[at] * product - CENTRE * pad_vector[step, row + 2, col + 2]
            following = rest * (2.0 / HALF) - pad_vector[step - 1, row + 2, col + 2]
            pad_vector[step + 1, row + 2, col + 2] = following

    for load in loads:
        load.wait()
    lane = lax.broadcasted_iota(jnp.int32, (col_count, slots), 1)
    square = (col_count, col_count)
    on_diagonal = lax.broadcasted_iota(jnp.int32, square, 0) == lax.broadcasted_iota(jnp.int32, square, 1)
    occupied = []
    for row in range(row_count):
        limits = jnp.where(
            on_diagonal, jnp.broadcast_to(counts_ref[row : row + 1].astype(jnp.float32), square), 0.0
        )
        limit = jnp.sum(limits, axis=1, keepdims=True)
        occupied.append((lane.astype(jnp.float32) < limit).astype(jnp.float32))
        live = occupied[row] > 0.0
        field_rows = (
            jnp.where(live, offsets_ref[0, row], FAR),
            jnp.where(live, offsets_ref[1, row], FAR),
            masses_ref[row],
            source_ref[row] * occupied[row],
        )
        source_ref[row] = field_rows[3]
        for col in range(col_count):
            for index in range(3):
                pad_fields[row + 1, col + 1, index : index + 1] = field_rows[index][col : col + 1]
            for index in range(2):
                centred = field_rows[index][col : col + 1] - MIDDLE
                deep_places[row + 2, col + 2, index : index + 1] = centred
        inverse_diag[row] = occupied[row].reshape(col_count, 1, slots)

    greeters = lambda low, high: low.astype(jnp.int32) + high.astype(jnp.int32)
    if near_only:
        count_x, count_y = greeters(low_x, high_x), greeters(low_y, high_y)
        further = greeters(here_y > 1, here_y < size_y - 2)
        pl.semaphore_wait(barrier, (count_x + 1) * (count_y + 1) - 1 + further)
    else:
        pl.semaphore_wait(barrier, device_count - 1)

    field_args = (pad_fields, 1, field_send, field_recv)
    start_halo(range(len(SIDES)), *field_args)
    deep_places_args = (deep_places, 2, deep_places_send, deep_places_recv)
    start_halo(range(len(SIDES)), *deep_places_args)

    def spread_place(row, col, place):
        own_x[row, col] = spread(offsets_ref[0, row, pl.ds(col, 1)])
        own_y[row, col] = spread(offsets_ref[1, row, pl.ds(col, 1)])

    all_columns(spread_place)

    def density_part(inside):
        def one(row, col, place):
            steps = steps_of(row, place, inside)

            def terms(rows):
                at_x, at_y = own_x[row, col, rows], own_y[row, col, rows]
                total = None
                for index, step_x, step_y in steps:
                    near = pad_fields[row + 1 + step_x, col + 1 + step_y]
                    offset_x = (step_x + near[0:1]) - at_x
                    offset_y = (step_y + near[1:2]) - at_y
                    falloff = jnp.maximum(1.0 - (offset_x * offset_x + offset_y * offset_y), 0.0)
                    squared = falloff * falloff
                    weights[row, col, index, rows] = squared
                    term = squared * falloff * near[2:3]
                    total = term if total is None else total + term
                return total

            return chunks(terms)

        return one

    def store_density_part(row, col, place):
        part[row, col] = density_part(True)(row, col, place)

    all_columns(store_density_part)
    end_halo(*field_args)

    def finish_density(row, col, place):
        density = 1.0 + (part[row, col] + density_part(False)(row, col, place))
        pad_density[row + 1, col + 1] = density
        deep_density[row + 2, col + 2] = density * (0.5 / PAIR_SCALE)
        density_ref[row, pl.ds(col, 1)] = density

    density_args = (pad_density, 1, density_send, density_recv)
    deep_density_args = (deep_density, 2, deep_density_send, deep_density_recv)
    edge_columns(finish_density)
    start_halo(LONG, *density_args)
    inner_columns(finish_density)
    start_halo(SHORT, *density_args)
    start_halo(range(len(SIDES)), *deep_density_args)

    def weight_part(inside):
        def one(row, col, place):
            steps = steps_of(row, place, inside)

            def terms(rows):
                here = own_density[row, col, rows]
                total = None
                for index, step_x, step_y in steps:
                    there = pad_density[row + 1 + step_x, col + 1 + step_y]
                    weight = weights[row, col, index, rows] * ((2.0 * PAIR_SCALE) / (here + there))
                    weights[row, col, index, rows] = weight
                    total = weight if total is None else total + weight
                return total

            return chunks(terms)

        return one

    def store_weight_part(row, col, place):
        own_density[row, col] = spread(pad_density[row + 1, col + 1])
        part[row, col] = weight_part(True)(row, col, place)

    all_columns(store_weight_part)
    end_halo(*deep_places_args)
    in_turn(spread_ring_places, set_ring_squares, ring[:READY])
    end_halo(*density_args)

    def finish_weights(row, col, place):
        occupied_row = inverse_diag[row, col]
        total = part[row, col] + weight_part(False)(row, col, place)
        diagonal = BASE_STIFF + occupied_row * total
        inverted = occupied_row / diagonal
        scaled = source_ref[row, pl.ds(col, 1)] * inverted
        diag_ref[row, pl.ds(col, 1)] = diagonal
        inverse_diag[row, col] = inverted
        vectors[0, row, pl.ds(col, 1)] = scaled
        pad_vector[0, row + 2, col + 2] = scaled

    def vector_args(step):
        depth = 2 if step in DEEP else 1
        return pad_vector.at[step], depth, vector_send.at[step], vector_recv.at[step]

    edge_columns(finish_weights)
    start_halo(LONG, *vector_args(0))
    inner_columns(finish_weights)
    start_halo(SHORT, *vector_args(0))

    def product_part(step, inside):
        def one(row, col, place):
            total = None
            for index, step_x, step_y in steps_of(row, place, inside):
                term = weights[row, col, index] * pad_vector[step, row + 2 + step_x, col + 2 + step_y]
                total = term if total is None else total + term
            return gathered(total)

        return one

    def store_product_part(step):
        def one(row, col, place):
            part[row, col] = product_part(step, True)(row, col, place)

        return one

    def finish_product(step):
        def one(row, col, place):
            if step - 1 in DEEP:
                product = product_part(step, None)(row, col, place)
            else:
                product = part[row, col] + product_part(step, False)(row, col, place)
            products[step, row, pl.ds(col, 1)] = product
            now = vectors[step, row, pl.ds(col, 1)]
            rest = inverse_diag[row, col] * product - CENTRE * now
            if step == 0:
                following = rest * (1.0 / HALF)
            else:
                following = rest * (2.0 / HALF) - vectors[step - 1, row, pl.ds(col, 1)]
            vectors[step + 1, row, pl.ds(col, 1)] = following
            if step + 1 < ITERS:
                pad_vector[step + 1, row + 2, col + 2] = following

        return one

    def set_image(step):
        for row in range(row_count):
            images[step, row] = diag_ref[row] * vectors[step, row] - products[step, row]

    def dot(left, right):
        zero = jnp.zeros((col_count, slots), jnp.float32)
        return tree([(left[row] * right[row], zero) for row in range(row_count)], add)

    def send_all(gather, send_sem, recv_sem):
        def one(index, step_x, step_y):
            return pltpu.make_async_remote_copy(
                src_ref=gather.at[0],
                dst_ref=gather.at[index],
                send_sem=send_sem.at[index],
                recv_sem=recv_sem.at[index],
                device_id=(ahead(here_x, step_x, size_x), ahead(here_y, step_y, size_y)),
                device_id_type=MESH,
            )

        return one

    def start_all(*args):
        for_peers(lambda *peer: send_all(*args)(*peer).start())

    def end_all(*args):
        for_peers(lambda *peer: send_all(*args)(*peer).wait_recv())

    def end_all_sends(*args):
        for_peers(lambda *peer: send_all(*args)(*peer).wait_send())

    early_args = (gather_early, early_send, early_recv)
    late_args = (gather_late, late_send, late_recv)
    peak_args = (gather_peak, peak_send, peak_recv)
    last = ITERS - 1
    group = slots // col_count
    entries = [("image", i, j) for j in range(last) for i in range(min(j + 1, last - 1))]
    entries += [("source", 0, j) for j in range(last)]
    late_entries = [("image", last - 1, last - 1), ("source", 0, last)]
    late_entries += [("image", i, last) for i in range(last)]
    entries += [None] * (-len(entries) % group) + late_entries
    groups = -(-len(entries) // group)
    first_late = groups - -(-len(late_entries) // group)

    def early_sums(chosen):
        filler = jnp.zeros((col_count, slots), jnp.float32)
        for at in chosen:
            rows = []
            for entry in entries[at * group : (at + 1) * group]:
                if entry is None:
                    rows.append((filler, filler))
                    continue
                kind, i, j = entry
                rows.append(dot(images.at[i] if kind == "image" else source_ref, vectors.at[j]))
            rows = rows + [(filler, filler)] * (group - len(rows))
            flat = [jnp.concatenate([pair[which] for pair in rows], axis=0).T for which in (0, 1)]
            slabs = [
                (flat[0][start : start + 8], flat[1][start : start + 8]) for start in range(0, slots, 8)
            ]
            pair = over_sublanes(tree(slabs, add), 8)
            gather_early[0, at : at + 1] = pair[0][0:1]
            gather_early[0, groups + at : groups + at + 1] = pair[1][0:1]

    def sum_lanes(pair):
        flat = [jnp.broadcast_to(part_of[0:1], (slots, slots)).T for part_of in pair]
        slabs = [(flat[0][start : start + 8], flat[1][start : start + 8]) for start in range(0, slots, 8)]
        return over_sublanes(tree(slabs, add), 8)

    def end_product(step):
        sends = step < last and step not in DEEP
        depth = 2 if step + 1 in DEEP else 1
        edge_columns(finish_product(step), depth)
        if sends:
            start_halo(LONG, *vector_args(step + 1))
        if step - 1 in DEEP and sends:
            finish_ring(step - 1, ring_middle)
        inner_columns(finish_product(step), depth)
        if sends:
            start_halo(SHORT, *vector_args(step + 1))
        if step < last:
            set_image(step)

    for step in range(last):
        if step - 1 not in DEEP:
            all_columns(store_product_part(step))
            set_ring_share(step)
            if step == DEEP[1]:
                early_sums(range(first_late))
            start_ring(step)
            end_halo(*vector_args(step))
        end_product(step)
        if step == last - 1:
            early_sums(range(first_late, groups))
            start_all(*early_args)
        if step in DEEP:
            finish_ring(step, ring_ends if step == DEEP[0] else ring)

    crossing = []
    for row in range(row_count):
        for col in range(col_count):
            place = "first" if col == 0 else "last" if col == col_count - 1 else "inner"
            inside = [index for index, _, _ in steps_of(row, place, True)]
            single = twice = None
            for index, (step_x, step_y) in enumerate(NEIGHBOUR_STEPS):
                if index in inside and (step_x, step_y) < (0, 0):
                    continue
                term = weights[row, col, index] * pad_vector[last, row + 2 + step_x, col + 2 + step_y]
                if index in inside and (step_x, step_y) > (0, 0):
                    twice = term if twice is None else twice + term
                else:
                    single = term if single is None else single + term
            total = single if twice is None else single + (twice + twice)
            total = total * spread(vectors[last, row, pl.ds(col, 1)])
            crossing.append(tree([total[start : start + 8] for start in range(0, slots, 8)], jnp.add))
    zero = jnp.zeros((8, slots), jnp.float32)
    pair = tree([(-one, zero) for one in crossing], add)
    for row in range(row_count):
        now = vectors[last, row]
        pair = add(pair, (diag_ref[row] * now * now, zero))
    pair = sum_lanes(over_sublanes(pair, 8))
    gather_late[0, 0:1] = pair[0][0:1]
    gather_late[0, 1:2] = pair[1][0:1]
    start_all(*late_args)

    end_product(last)
    end_all(*early_args)
    sums = {}
    for at in range(groups):
        pair = tree(
            [
                (gather_early[device, at : at + 1], gather_early[device, groups + at : groups + at + 1])
                for device in range(device_count)
            ],
            add,
        )
        flat = [spread(part_of) for part_of in pair]
        for index, entry in enumerate(entries[at * group : (at + 1) * group]):
            if entry is None:
                continue
            rows = slice(index * col_count, (index + 1) * col_count)
            sums[entry] = tidy(over_sublanes((flat[0][rows], flat[1][rows]), col_count))
    matrix = lambda i, j: sums["image", min(i, j), max(i, j)]

    zero = jnp.zeros((col_count, slots), jnp.float32)
    nothing = (zero, zero)
    unit = (zero + 1.0, zero)
    number = lambda value: (zero + value, zero)
    inverses, factors, directions, shares = [], {}, [], []
    kept_last = None
    for k in range(ITERS):
        scaled = {}
        for j in range(k):
            value = matrix(k, j)
            for i in range(j):
                value = sub(value, mul(scaled[i], factors[j, i]))
            scaled[j] = value
            factors[k, j] = mul(value, inverses[j])
        target = sums["source", 0, k]
        for j in range(k):
            target = sub(target, mul(factors[k, j], shares[j][0]))
        removed = nothing
        for j in range(k):
            removed = tidy(add(removed, mul(scaled[j], factors[k, j])))
        direction = [nothing] * k + [unit]
        for j in range(k):
            for i in range(j + 1):
                direction[i] = sub(direction[i], mul(factors[k, j], directions[j][i]))
        directions.append(direction)
        if k < last:
            pivot = sub(matrix(k, k), removed)
            inverses.append(inverse(pivot))
            shares.append((target, mul(target, inverses[k])))
        else:
            kept_last = (target, removed)

    def applied(direction):
        count = len(direction)
        padded = direction + [nothing, nothing]
        out = []
        for i in range(count + 1):
            value = mul(padded[i], number(1.0 - CENTRE))
            if i:
                value = sub(value, mul(padded[i - 1], number(HALF if i == 1 else HALF / 2)))
            out.append(sub(value, mul(padded[i + 1], number(HALF / 2))))
        return out

    def combined(coefficients, row):
        return tree([value[0] * vectors[i, row] for i, value in enumerate(coefficients)], jnp.add)

    solution = [nothing] * ITERS
    remainder = [unit] + [nothing] * ITERS
    peak_rows = []

    def largest(rows):
        peak = tree([jnp.abs(one) for one in rows], jnp.maximum)
        return jnp.max(jnp.max(peak, axis=0, keepdims=True), axis=1, keepdims=True)

    for k in range(last):
        share = shares[k][1]
        image = applied(directions[k])
        for i, value in enumerate(directions[k]):
            solution[i] = tidy(add(solution[i], mul(share, value)))
        for i, value in enumerate(image):
            remainder[i] = sub(remainder[i], mul(share, value))
        rows = [diag_ref[row] * combined(remainder[: k + 2], row) for row in range(row_count)]
        peak_rows.append(largest(rows))
    residual_rows = rows
    image = applied(directions[last])
    solution_rows = [combined(solution[:last], row) for row in range(row_count)]
    direction_rows = [combined(directions[last], row) for row in range(row_count)]
    image_rows = [diag_ref[row] * combined(image, row) for row in range(row_count)]

    end_all(*late_args)
    pair = tree(
        [(gather_late[device, 0:1], gather_late[device, 1:2]) for device in range(device_count)], add
    )
    target, removed = kept_last
    pivot = sub(tidy(pair), (removed[0][0:1], removed[1][0:1]))
    share = target[0][0:1] / pivot[0]
    for row in range(row_count):
        residual_rows[row] = residual_rows[row] - share * image_rows[row]
        residual_ref[row] = residual_rows[row]
        pressure_ref[row] = solution_rows[row] + share * direction_rows[row]
    peak_rows.append(largest(residual_rows))
    lane = lax.broadcasted_iota(jnp.int32, (1, slots), 1)
    packed = jnp.zeros((1, slots), jnp.float32)
    for k in range(ITERS):
        packed = jnp.where(lane == k, peak_rows[k], packed)
    gather_peak[0] = packed
    start_all(*peak_args)

    end_sends(*field_args)
    end_sends(*density_args)
    end_sends(*deep_places_args)
    end_sends(*deep_density_args)
    for step in range(ITERS):
        if step - 1 not in DEEP:
            end_sends(*vector_args(step))
    end_all_sends(*early_args)
    end_all_sends(*late_args)
    end_all(*peak_args)
    peaks_ref[...] = tree([gather_peak[device] for device in range(device_count)], jnp.maximum)
    end_all_sends(*peak_args)


def write_out(density_ref, pressure_ref, residual_ref, peaks_ref, *rest):
    outs, packed_ref, sems = rest[:4], rest[4], rest[5]
    packed_ref[...] = peaks_ref[0, : packed_ref.shape[0]]
    copies = [
        pltpu.make_async_copy(source, target, sems.at[index])
        for index, (source, target) in enumerate(
            zip((density_ref, pressure_ref, residual_ref, packed_ref), outs)
        )
    ]
    for copy in copies:
        copy.start()
    for copy in copies:
        copy.wait()


def body(size_x, size_y, offsets, masses, counts, source):
    row_count, col_count, slots = masses.shape
    devices = size_x * size_y
    padded = (row_count + 2, col_count + 2)
    deep = (row_count + 4, col_count + 4)
    ring_count = padded[0] * padded[1] - row_count * col_count
    block = (row_count, col_count, slots)
    dma, f32, sides = pltpu.SemaphoreType.DMA, jnp.float32, len(SIDES)
    scratch = lambda *shape: pltpu.VMEM(shape, f32)
    group = slots // col_count
    early_rows = 2 * (-(-((ITERS - 1) * (ITERS + 2) // 2 - 1) // group) + -(-(ITERS + 1) // group))
    weight_bytes = 4 * row_count * col_count * len(NEIGHBOUR_STEPS) * slots * slots
    vmem = pl.BlockSpec(memory_space=pltpu.VMEM)
    hbm = pl.BlockSpec(memory_space=pltpu.HBM)
    shaped = jax.ShapeDtypeStruct(block, f32)
    results = pl.pallas_call(
        functools.partial(kernel, size_x, size_y, row_count, col_count),
        out_shape=(shaped, shaped, shaped, jax.ShapeDtypeStruct((1, slots), f32)),
        in_specs=[hbm] * 4,
        out_specs=(vmem,) * 4,
        scratch_shapes=[
            scratch(2, *block), scratch(*block), pltpu.VMEM((row_count, col_count), jnp.int32),
            scratch(*block), dma((4,)),
            scratch(*padded, 4, slots), scratch(*padded, 1, slots), scratch(ITERS, *deep, 1, slots),
            scratch(row_count, col_count, len(NEIGHBOUR_STEPS), slots, slots),
            scratch(row_count, col_count, slots, slots),
            scratch(row_count, col_count, slots, slots),
            scratch(row_count, col_count, slots, slots),
            scratch(row_count, col_count, 1, slots),
            scratch(row_count, col_count, 1, slots),
            scratch(*block),
            scratch(ITERS + 1, *block), scratch(ITERS, *block), scratch(ITERS, *block),
            scratch(*deep, 2, slots), scratch(*deep, 1, slots),
            scratch(ring_count, len(NEIGHBOUR_STEPS), slots, slots), scratch(ring_count, 1, slots),
            scratch(ring_count, 1, slots), scratch(ring_count, 3, slots, slots),
            scratch(devices, early_rows, slots), scratch(devices, 2, slots), scratch(devices, 1, slots),
            dma((sides,)), dma((sides,)), dma((sides,)), dma((sides,)),
            dma((ITERS, sides)), dma((ITERS, sides)),
            dma((devices,)), dma((devices,)), dma((devices,)), dma((devices,)),
            dma((devices,)), dma((devices,)),
            dma((sides,)), dma((sides,)), dma((sides,)), dma((sides,)),
        ],
        compiler_params=pltpu.CompilerParams(
            collective_id=0, has_side_effects=True, vmem_limit_bytes=4 * weight_bytes
        ),
    )(*(pltpu.with_memory_space_constraint(one, pltpu.HBM) for one in (offsets, masses, counts, source)))
    return pl.pallas_call(
        write_out,
        out_shape=(shaped, shaped, shaped, jax.ShapeDtypeStruct((ITERS,), f32)),
        in_specs=[vmem] * 4,
        out_specs=(hbm,) * 4,
        scratch_shapes=[scratch(ITERS), dma((4,))],
        compiler_params=pltpu.CompilerParams(vmem_limit_bytes=weight_bytes),
    )(*results)


def solution(mesh):
    in_specs = (P(None, "gx", "gy", None), P("gx", "gy", None), P("gx", "gy"), P("gx", "gy", None))
    out_specs = (P("gx", "gy", None), P("gx", "gy", None), P("gx", "gy", None), P())
    return jax.shard_map(
        functools.partial(body, mesh.shape["gx"], mesh.shape["gy"]),
        mesh=mesh, in_specs=in_specs, out_specs=out_specs, check_vma=False,
    )
```

```python
import functools

import jax
import jax.numpy as jnp
from jax import lax
from jax.experimental import pallas as pl
from jax.experimental.pallas import tpu as pltpu
from jax.sharding import PartitionSpec as P

ITERS = 5
BASE_STIFF = 0.5
PAIR_SCALE = 0.05
NEIGHBOUR_STEPS = [(step_x, step_y) for step_x in (-1, 0, 1) for step_y in (-1, 0, 1)]
SIDES = [step for step in NEIGHBOUR_STEPS if step != (0, 0)]
MESH = pl.DeviceIdType.MESH
FAR = 64.0
CENTRE, HALF = 0.4375, 0.5
CHUNK = 64
DEEP = (1, 3)
SHORT_WAY, LONG_WAY = "short", "long"
READY = 9
FIRST = 13
MIDDLE = 0.5


def two_sum(a, b):
    total = a + b
    part = total - a
    return total, (a - (total - part)) + (b - part)


def add(a, b):
    high, low = two_sum(a[0], b[0])
    return high, low + (a[1] + b[1])


def tidy(a):
    high = a[0] + a[1]
    return high, a[1] - (high - a[0])


def halves(a):
    wide = a * 4097.0
    high = wide - (wide - a)
    return high, a - high


def mul(a, b):
    a_high, a_low = halves(a[0])
    b_high, b_low = halves(b[0])
    product = a[0] * b[0]
    rest = ((a_high * b_high - product) + (a_high * b_low + a_low * b_high)) + a_low * b_low
    return tidy((product, rest + (a[0] * b[1] + a[1] * b[0])))


def neg(a):
    return -a[0], -a[1]


def sub(a, b):
    return tidy(add(a, neg(b)))


def inverse(a):
    first = 1.0 / a[0]
    start = (first, jnp.zeros_like(first))
    one = (jnp.ones_like(first), jnp.zeros_like(first))
    rest = sub(one, mul(start, a))
    return tidy((first, rest[0] * first))


def tree(items, combine):
    items = list(items)
    while len(items) > 1:
        paired = [combine(items[at], items[at + 1]) for at in range(0, len(items) - 1, 2)]
        items = paired + items[len(paired) * 2 :]
    return items[0]


def over_sublanes(pair, rows):
    shift = rows // 2
    while shift:
        pair = add(pair, tuple(pltpu.roll(part, shift, 0) for part in pair))
        shift //= 2
    return pair


def kernel(
    size_x, size_y, row_count, col_count,
    offsets_hbm, masses_hbm, counts_hbm, source_hbm,
    density_ref, pressure_ref, residual_ref, peaks_ref,
    offsets_ref, masses_ref, counts_ref, source_ref, load_sem,
    pad_fields, pad_density, pad_vector, weights, own_x, own_y, own_density,
    part, inverse_diag, diag_ref, vectors, products, images,
    deep_places, deep_density, ring_weights, ring_inverse, ring_part, ring_own,
    gather_early, gather_late, gather_peak,
    field_send, field_recv, density_send, density_recv, vector_send, vector_recv,
    early_send, early_recv, late_send, late_recv, peak_send, peak_recv,
    deep_places_send, deep_places_recv, deep_density_send, deep_density_recv,
):
    here_x, here_y = lax.axis_index("gx"), lax.axis_index("gy")
    device_count = size_x * size_y
    slots = masses_ref.shape[-1]

    loads = [
        pltpu.make_async_copy(source, target, load_sem.at[index])
        for index, (source, target) in enumerate((
            (offsets_hbm, offsets_ref), (masses_hbm, masses_ref),
            (counts_hbm, counts_ref), (source_hbm, source_ref),
        ))
    ]
    for load in loads:
        load.start()

    low_x, high_x = (here_x > 0), (here_x < size_x - 1)
    low_y, high_y = (here_y > 0), (here_y < size_y - 1)

    def on_side(step_x, step_y, action):
        conditions = []
        if step_x:
            conditions.append({1: high_x, -1: low_x}[step_x])
        if step_y:
            conditions.append({1: high_y, -1: low_y}[step_y])
        condition = conditions[0]
        for other in conditions[1:]:
            condition = jnp.logical_and(condition, other)
        pl.when(condition)(action)

    def ahead(here, step, size):
        there = here + step
        return jnp.where(there >= size, there - size, there)

    def for_peers(action):
        def turned(step_y):
            return jnp.where(here_y < size_y // 2, size_y - step_y, step_y)

        if device_count <= 64:
            for step_y in range(1, size_y):
                for step_x in range(size_x - 1, -1, -1):
                    action(step_x * size_y + turned(step_y), step_x, turned(step_y))
            for step_x in range(1, size_x):
                action(step_x * size_y, step_x, 0)
        else:
            def one(index, carry):
                action(index, lax.div(index, size_y), lax.rem(index, size_y))
                return carry

            lax.fori_loop(1, device_count, one, 0)

    barrier = pltpu.get_barrier_semaphore()

    def greet(device):
        pl.semaphore_signal(barrier, inc=1, device_id=device, device_id_type=MESH)

    near_only = size_x <= ITERS + 2 and size_y <= ITERS + 3
    if near_only:
        for step_x, step_y in SIDES:
            on_side(step_x, step_y, functools.partial(greet, (here_x + step_x, here_y + step_y)))
        pl.when(here_y > 1)(lambda: greet((here_x, here_y - 2)))
        pl.when(here_y < size_y - 2)(lambda: greet((here_x, here_y + 2)))
    else:
        for_peers(lambda index, step_x, step_y: greet(
            (ahead(here_x, step_x, size_x), ahead(here_y, step_y, size_y))
        ))

    def fill(ref, value):
        ref[...] = jnp.full(ref.shape, value, jnp.float32)

    def fill_outside(axis, start):
        def at(margin):
            span = pl.ds(start + margin if start > 0 else 0, margin)
            return (span, slice(None)) if axis == 0 else (slice(None), span)

        fill(pad_fields.at[at(1)], FAR)
        fill(pad_density.at[at(1)], 1.0)
        fill(deep_places.at[at(2)], FAR)
        fill(deep_density.at[at(2)], 1.0)
        for step in range(ITERS):
            fill(pad_vector.at[(step,) + at(2)], 0.0)

    pl.when(jnp.logical_not(low_x))(lambda: fill_outside(0, 0))
    pl.when(jnp.logical_not(high_x))(lambda: fill_outside(0, row_count))
    pl.when(jnp.logical_not(low_y))(lambda: fill_outside(1, 0))
    pl.when(jnp.logical_not(high_y))(lambda: fill_outside(1, col_count))

    def halo_copy(side, pad, depth, send_sem, recv_sem):
        step_x, step_y = SIDES[side]
        margin = (pad.shape[0] - row_count) // 2

        def inner(step, count):
            start = margin + count - depth if step > 0 else margin
            return pl.ds(start, depth if step else count)

        def outer(step, count):
            start = {1: margin - depth, -1: margin + count, 0: margin}[step]
            return pl.ds(start, depth if step else count)

        return pltpu.make_async_remote_copy(
            src_ref=pad.at[inner(step_x, row_count), inner(step_y, col_count)],
            dst_ref=pad.at[outer(step_x, row_count), outer(step_y, col_count)],
            send_sem=send_sem.at[side],
            recv_sem=recv_sem.at[side],
            device_id=(here_x + step_x, here_y + step_y),
            device_id_type=MESH,
        )

    LONG = [side for side, step in enumerate(SIDES) if step[1]]
    SHORT = [side for side, step in enumerate(SIDES) if not step[1]]

    def start_halo(sides, *args):
        for side in sides:
            on_side(*SIDES[side], lambda side=side: halo_copy(side, *args).start())

    def end_halo(*args, sides=range(len(SIDES))):
        for side in sides:
            step_x, step_y = SIDES[side]
            on_side(-step_x, -step_y, lambda side=side: halo_copy(side, *args).wait_recv())

    def end_sends(*args):
        for side, (step_x, step_y) in enumerate(SIDES):
            on_side(step_x, step_y, lambda side=side: halo_copy(side, *args).wait_send())

    def steps_of(row, place, inside):
        def is_inside(step_x, step_y):
            if not 0 <= row + step_x < row_count:
                return False
            return not (place == "first" and step_y < 0 or place == "last" and step_y > 0)

        def is_wanted(step_x, step_y):
            if inside in (SHORT_WAY, LONG_WAY):
                long_way = place == "first" and step_y < 0 or place == "last" and step_y > 0
                return not is_inside(step_x, step_y) and long_way == (inside == LONG_WAY)
            return inside is None or is_inside(step_x, step_y) == inside

        return [
            (index, step_x, step_y)
            for index, (step_x, step_y) in enumerate(NEIGHBOUR_STEPS)
            if is_wanted(step_x, step_y)
        ]

    def columns(action, chosen):
        for col in chosen:
            place = "first" if col == 0 else "last" if col == col_count - 1 else "inner"
            for row in range(row_count):
                action(row, col, place)

    def edge_columns(action, depth=1):
        columns(action, [col for col in range(col_count) if not depth <= col < col_count - depth])

    def inner_columns(action, depth=1):
        columns(action, range(depth, col_count - depth))

    def all_columns(action):
        edge_columns(action)
        inner_columns(action)

    def spread(row):
        return jnp.broadcast_to(row, (slots, slots)).T

    def gathered(total):
        return jnp.sum(total.T, axis=0, keepdims=True)

    def chunks(terms):
        return gathered(jnp.concatenate(
            [terms(pl.ds(start, CHUNK)) for start in range(0, slots, CHUNK)], axis=0
        ))

    wide = col_count + 2
    ring = [(col + 1, -1, col) for col in range(-1, col_count + 1)]
    ring += [(wide + col + 1, row_count, col) for col in range(-1, col_count + 1)]
    ring += [(2 * wide + 2 * row, row, -1) for row in range(row_count)]
    ring += [(2 * wide + 2 * row + 1, row, col_count) for row in range(row_count)]

    ring_middle = [cell for cell in ring if 3 <= cell[2] < col_count - 3]
    ring_ends = [cell for cell in ring if cell not in ring_middle]
    ring_short = [
        cell for cell in ring if cell[1] in (-1, row_count) and 1 <= cell[2] < col_count - 1
    ]
    ring_long = [cell for cell in ring if cell not in ring_short]
    ring_at = {(row, col): at for at, row, col in ring}

    def known(at, row, col):
        out = []
        for index, (step_x, step_y) in enumerate(NEIGHBOUR_STEPS):
            cell = (row + step_x, col + step_y)
            back = len(NEIGHBOUR_STEPS) - 1 - index
            if 0 <= cell[0] < row_count and 0 <= cell[1] < col_count:
                out.append(("own", cell, back))
            elif cell in ring_at and order[ring_at[cell]] < order[at]:
                out.append(("ring", ring_at[cell], back))
            else:
                out.append(None)
        return out

    order = {at: place for place, (at, _, _) in enumerate(ring)}

    def spread_ring_places(at, row, col):
        places = deep_places[row + 2, col + 2]
        ring_own[at, 0] = spread(2.0 * places[0:1])
        ring_own[at, 1] = spread(2.0 * places[1:2])

    def spread_ring(at, row, col):
        if order[at] >= READY:
            spread_ring_places(at, row, col)
        ring_own[at, 2] = spread(deep_density[row + 2, col + 2])

    def in_turn(prepare, action, cells):
        prepare(*cells[0])
        for place, cell in enumerate(cells):
            if place + 1 < len(cells):
                prepare(*cells[place + 1])
            action(*cell)

    def ring_squares(at, row, col, rows):
        twice_x, twice_y = ring_own[at, 0, rows], ring_own[at, 1, rows]
        rest = 1.0 - 0.25 * (twice_x * twice_x + twice_y * twice_y)

        def one(index):
            step_x, step_y = NEIGHBOUR_STEPS[index]
            near = deep_places[row + 2 + step_x, col + 2 + step_y]
            near_x, near_y = near[0:1] + step_x, near[1:2] + step_y
            near_rest = near_x * near_x + near_y * near_y
            falloff = (rest - near_rest) + (twice_x * near_x + twice_y * near_y)
            falloff = jnp.maximum(falloff, 0.0)
            return falloff * falloff

        return one

    def parts():
        return [slice(start, start + CHUNK) for start in range(0, slots, CHUNK)]

    def set_ring_squares(at, row, col):
        for rows in parts():
            squares = ring_squares(at, row, col, rows)
            for index, found in enumerate(known(at, row, col)):
                if found is None:
                    ring_weights[at, index, rows] = squares(index)

    def set_ring_weights(at, row, col):
        ready = order[at] < READY
        totals = []
        turned = {}
        for index, found in enumerate(known(at, row, col)):
            if found is None:
                continue
            kind, cell, back = found
            if kind == "own":
                turned[index] = weights[cell[0], cell[1], back].T
                places = deep_places[cell[0] + 2, cell[1] + 2]
                live = (places[0:1] < FAR / 2).astype(jnp.float32)
            else:
                turned[index] = ring_weights[cell, back].T
                live = 1.0
            ring_weights[at, index] = turned[index]
            turned[index] = turned[index] * live
        for rows in parts():
            squares = None if ready else ring_squares(at, row, col, rows)
            here = ring_own[at, 2, rows]
            total = None
            for index, (step_x, step_y) in enumerate(NEIGHBOUR_STEPS):
                if index in turned:
                    weight = turned[index][rows]
                else:
                    there = deep_density[row + 2 + step_x, col + 2 + step_y]
                    square = ring_weights[at, index, rows] if ready else squares(index)
                    weight = square / (here + there)
                    ring_weights[at, index, rows] = weight
                total = weight if total is None else total + weight
            totals.append(total)
        total = gathered(jnp.concatenate(totals, axis=0))
        live = (deep_places[row + 2, col + 2][0:1] < FAR / 2).astype(jnp.float32)
        ring_inverse[at] = live / (BASE_STIFF + live * total)

    def set_ring_share(step):
        if step > DEEP[0]:
            return
        if step == 0:
            end_halo(*deep_density_args)
        share = ring[:FIRST] if step == 0 else ring[FIRST:]
        in_turn(spread_ring, set_ring_weights, share)

    def ring_product(step, at, row, col, inside):
        total = None
        for index, (step_x, step_y) in enumerate(NEIGHBOUR_STEPS):
            own = 0 <= row + step_x < row_count and 0 <= col + step_y < col_count
            if inside is None or own == inside:
                term = ring_weights[at, index] * pad_vector[step, row + 2 + step_x, col + 2 + step_y]
                total = term if total is None else total + term
        return gathered(total)

    def start_ring(step):
        if step == DEEP[1]:
            for at, row, col in ring:
                ring_part[at] = ring_product(step, at, row, col, True)

    def finish_ring(step, cells):
        for at, row, col in cells:
            if step == DEEP[1]:
                product = ring_part[at] + ring_product(step, at, row, col, False)
            else:
                product = ring_product(step, at, row, col, None)
            rest = ring_inverse[at] * product - CENTRE * pad_vector[step, row + 2, col + 2]
            following = rest * (2.0 / HALF) - pad_vector[step - 1, row + 2, col + 2]
            pad_vector[step + 1, row + 2, col + 2] = following

    for load in loads:
        load.wait()
    lane = lax.broadcasted_iota(jnp.int32, (col_count, slots), 1)
    square = (col_count, col_count)
    on_diagonal = lax.broadcasted_iota(jnp.int32, square, 0) == lax.broadcasted_iota(jnp.int32, square, 1)
    occupied = []
    for row in range(row_count):
        limits = jnp.where(
            on_diagonal, jnp.broadcast_to(counts_ref[row : row + 1].astype(jnp.float32), square), 0.0
        )
        limit = jnp.sum(limits, axis=1, keepdims=True)
        occupied.append((lane.astype(jnp.float32) < limit).astype(jnp.float32))
        live = occupied[row] > 0.0
        field_rows = (
            jnp.where(live, offsets_ref[0, row], FAR),
            jnp.where(live, offsets_ref[1, row], FAR),
            masses_ref[row],
            source_ref[row] * occupied[row],
        )
        source_ref[row] = field_rows[3]
        for col in range(col_count):
            for index in range(3):
                pad_fields[row + 1, col + 1, index : index + 1] = field_rows[index][col : col + 1]
            for index in range(2):
                centred = field_rows[index][col : col + 1] - MIDDLE
                deep_places[row + 2, col + 2, index : index + 1] = centred
        inverse_diag[row] = occupied[row].reshape(col_count, 1, slots)

    greeters = lambda low, high: low.astype(jnp.int32) + high.astype(jnp.int32)
    if near_only:
        count_x, count_y = greeters(low_x, high_x), greeters(low_y, high_y)
        further = greeters(here_y > 1, here_y < size_y - 2)
        pl.semaphore_wait(barrier, (count_x + 1) * (count_y + 1) - 1 + further)
    else:
        pl.semaphore_wait(barrier, device_count - 1)

    field_args = (pad_fields, 1, field_send, field_recv)
    start_halo(range(len(SIDES)), *field_args)
    deep_places_args = (deep_places, 2, deep_places_send, deep_places_recv)
    start_halo(range(len(SIDES)), *deep_places_args)

    def spread_place(row, col, place):
        own_x[row, col] = spread(offsets_ref[0, row, pl.ds(col, 1)])
        own_y[row, col] = spread(offsets_ref[1, row, pl.ds(col, 1)])

    all_columns(spread_place)

    def density_part(inside):
        def one(row, col, place):
            steps = steps_of(row, place, inside)

            def terms(rows):
                at_x, at_y = own_x[row, col, rows], own_y[row, col, rows]
                total = None
                for index, step_x, step_y in steps:
                    near = pad_fields[row + 1 + step_x, col + 1 + step_y]
                    offset_x = (step_x + near[0:1]) - at_x
                    offset_y = (step_y + near[1:2]) - at_y
                    falloff = jnp.maximum(1.0 - (offset_x * offset_x + offset_y * offset_y), 0.0)
                    squared = falloff * falloff
                    weights[row, col, index, rows] = squared
                    term = squared * falloff * near[2:3]
                    total = term if total is None else total + term
                return total

            return chunks(terms)

        return one

    def store_density_part(row, col, place):
        part[row, col] = density_part(True)(row, col, place)

    def add_density_part(row, col, place):
        part[row, col] = part[row, col] + density_part(SHORT_WAY)(row, col, place)

    all_columns(store_density_part)
    end_halo(*field_args, sides=SHORT)
    edge_columns(add_density_part)
    end_halo(*field_args, sides=LONG)

    def finish_density(row, col, place):
        rest = density_part(False if place == "inner" else LONG_WAY)(row, col, place)
        density = 1.0 + (part[row, col] + rest)
        pad_density[row + 1, col + 1] = density
        deep_density[row + 2, col + 2] = density * (0.5 / PAIR_SCALE)
        density_ref[row, pl.ds(col, 1)] = density

    density_args = (pad_density, 1, density_send, density_recv)
    deep_density_args = (deep_density, 2, deep_density_send, deep_density_recv)
    edge_columns(finish_density)
    start_halo(LONG, *density_args)
    inner_columns(finish_density)
    start_halo(SHORT, *density_args)
    start_halo(range(len(SIDES)), *deep_density_args)

    def weight_part(inside):
        def one(row, col, place):
            steps = steps_of(row, place, inside)

            def terms(rows):
                here = own_density[row, col, rows]
                total = None
                for index, step_x, step_y in steps:
                    there = pad_density[row + 1 + step_x, col + 1 + step_y]
                    weight = weights[row, col, index, rows] * ((2.0 * PAIR_SCALE) / (here + there))
                    weights[row, col, index, rows] = weight
                    total = weight if total is None else total + weight
                return total

            return chunks(terms)

        return one

    def store_weight_part(row, col, place):
        own_density[row, col] = spread(pad_density[row + 1, col + 1])
        part[row, col] = weight_part(True)(row, col, place)

    all_columns(store_weight_part)
    end_halo(*deep_places_args)
    in_turn(spread_ring_places, set_ring_squares, ring[:READY])
    end_halo(*density_args)

    def finish_weights(row, col, place):
        occupied_row = inverse_diag[row, col]
        total = part[row, col] + weight_part(False)(row, col, place)
        diagonal = BASE_STIFF + occupied_row * total
        inverted = occupied_row / diagonal
        scaled = source_ref[row, pl.ds(col, 1)] * inverted
        diag_ref[row, pl.ds(col, 1)] = diagonal
        inverse_diag[row, col] = inverted
        vectors[0, row, pl.ds(col, 1)] = scaled
        pad_vector[0, row + 2, col + 2] = scaled

    def vector_args(step):
        depth = 2 if step in DEEP else 1
        return pad_vector.at[step], depth, vector_send.at[step], vector_recv.at[step]

    edge_columns(finish_weights)
    start_halo(LONG, *vector_args(0))
    inner_columns(finish_weights)
    start_halo(SHORT, *vector_args(0))

    def product_part(step, inside):
        def one(row, col, place):
            total = None
            for index, step_x, step_y in steps_of(row, place, inside):
                term = weights[row, col, index] * pad_vector[step, row + 2 + step_x, col + 2 + step_y]
                total = term if total is None else total + term
            return gathered(total)

        return one

    def store_product_part(step):
        def one(row, col, place):
            part[row, col] = product_part(step, True)(row, col, place)

        return one

    def finish_product(step):
        def one(row, col, place):
            if step - 1 in DEEP:
                product = product_part(step, None)(row, col, place)
            else:
                product = part[row, col] + product_part(step, False)(row, col, place)
            products[step, row, pl.ds(col, 1)] = product
            now = vectors[step, row, pl.ds(col, 1)]
            rest = inverse_diag[row, col] * product - CENTRE * now
            if step == 0:
                following = rest * (1.0 / HALF)
            else:
                following = rest * (2.0 / HALF) - vectors[step - 1, row, pl.ds(col, 1)]
            vectors[step + 1, row, pl.ds(col, 1)] = following
            if step + 1 < ITERS:
                pad_vector[step + 1, row + 2, col + 2] = following

        return one

    def set_image(step):
        for row in range(row_count):
            images[step, row] = diag_ref[row] * vectors[step, row] - products[step, row]

    def dot(left, right):
        zero = jnp.zeros((col_count, slots), jnp.float32)
        return tree([(left[row] * right[row], zero) for row in range(row_count)], add)

    def send_all(gather, send_sem, recv_sem):
        def one(index, step_x, step_y):
            return pltpu.make_async_remote_copy(
                src_ref=gather.at[0],
                dst_ref=gather.at[index],
                send_sem=send_sem.at[index],
                recv_sem=recv_sem.at[index],
                device_id=(ahead(here_x, step_x, size_x), ahead(here_y, step_y, size_y)),
                device_id_type=MESH,
            )

        return one

    def start_all(*args):
        for_peers(lambda *peer: send_all(*args)(*peer).start())

    def end_all(*args):
        for_peers(lambda *peer: send_all(*args)(*peer).wait_recv())

    def end_all_sends(*args):
        for_peers(lambda *peer: send_all(*args)(*peer).wait_send())

    early_args = (gather_early, early_send, early_recv)
    late_args = (gather_late, late_send, late_recv)
    peak_args = (gather_peak, peak_send, peak_recv)
    last = ITERS - 1
    group = slots // col_count
    entries = [("image", i, j) for j in range(last) for i in range(min(j + 1, last - 1))]
    entries += [("source", 0, j) for j in range(last)]
    late_entries = [("image", last - 1, last - 1), ("source", 0, last)]
    late_entries += [("image", i, last) for i in range(last)]
    entries += [None] * (-len(entries) % group) + late_entries
    groups = -(-len(entries) // group)
    first_late = groups - -(-len(late_entries) // group)

    def early_sums(chosen):
        filler = jnp.zeros((col_count, slots), jnp.float32)
        for at in chosen:
            rows = []
            for entry in entries[at * group : (at + 1) * group]:
                if entry is None:
                    rows.append((filler, filler))
                    continue
                kind, i, j = entry
                rows.append(dot(images.at[i] if kind == "image" else source_ref, vectors.at[j]))
            rows = rows + [(filler, filler)] * (group - len(rows))
            flat = [jnp.concatenate([pair[which] for pair in rows], axis=0).T for which in (0, 1)]
            slabs = [
                (flat[0][start : start + 8], flat[1][start : start + 8]) for start in range(0, slots, 8)
            ]
            pair = over_sublanes(tree(slabs, add), 8)
            gather_early[0, at : at + 1] = pair[0][0:1]
            gather_early[0, groups + at : groups + at + 1] = pair[1][0:1]

    def sum_lanes(pair):
        flat = [jnp.broadcast_to(part_of[0:1], (slots, slots)).T for part_of in pair]
        slabs = [(flat[0][start : start + 8], flat[1][start : start + 8]) for start in range(0, slots, 8)]
        return over_sublanes(tree(slabs, add), 8)

    def end_product(step):
        sends = step < last and step not in DEEP
        depth = 2 if step + 1 in DEEP else 1
        if step == DEEP[1]:
            inner_columns(finish_product(step), depth)
            finish_ring(step, ring_short)
            end_halo(*vector_args(step), sides=LONG)
        edge_columns(finish_product(step), depth)
        if sends:
            start_halo(LONG, *vector_args(step + 1))
        if step - 1 in DEEP and sends:
            finish_ring(step - 1, ring_middle)
        if step != DEEP[1]:
            inner_columns(finish_product(step), depth)
        if sends:
            start_halo(SHORT, *vector_args(step + 1))
        if step < last:
            set_image(step)

    for step in range(last):
        if step - 1 not in DEEP:
            all_columns(store_product_part(step))
            set_ring_share(step)
            if step == DEEP[1]:
                early_sums(range(first_late))
            start_ring(step)
            if step == DEEP[1]:
                end_halo(*vector_args(step), sides=SHORT)
            else:
                end_halo(*vector_args(step))
        end_product(step)
        if step == last - 1:
            early_sums(range(first_late, groups))
            start_all(*early_args)
        if step in DEEP:
            finish_ring(step, ring_ends if step == DEEP[0] else ring_long)

    crossing = []
    for row in range(row_count):
        for col in range(col_count):
            place = "first" if col == 0 else "last" if col == col_count - 1 else "inner"
            inside = [index for index, _, _ in steps_of(row, place, True)]
            single = twice = None
            for index, (step_x, step_y) in enumerate(NEIGHBOUR_STEPS):
                if index in inside and (step_x, step_y) < (0, 0):
                    continue
                term = weights[row, col, index] * pad_vector[last, row + 2 + step_x, col + 2 + step_y]
                if index in inside and (step_x, step_y) > (0, 0):
                    twice = term if twice is None else twice + term
                else:
                    single = term if single is None else single + term
            total = single if twice is None else single + (twice + twice)
            total = total * spread(vectors[last, row, pl.ds(col, 1)])
            crossing.append(tree([total[start : start + 8] for start in range(0, slots, 8)], jnp.add))
    zero = jnp.zeros((8, slots), jnp.float32)
    pair = tree([(-one, zero) for one in crossing], add)
    for row in range(row_count):
        now = vectors[last, row]
        pair = add(pair, (diag_ref[row] * now * now, zero))
    pair = sum_lanes(over_sublanes(pair, 8))
    gather_late[0, 0:1] = pair[0][0:1]
    gather_late[0, 1:2] = pair[1][0:1]
    start_all(*late_args)

    end_product(last)
    end_all(*early_args)
    sums = {}
    for at in range(groups):
        pair = tree(
            [
                (gather_early[device, at : at + 1], gather_early[device, groups + at : groups + at + 1])
                for device in range(device_count)
            ],
            add,
        )
        flat = [spread(part_of) for part_of in pair]
        for index, entry in enumerate(entries[at * group : (at + 1) * group]):
            if entry is None:
                continue
            rows = slice(index * col_count, (index + 1) * col_count)
            sums[entry] = tidy(over_sublanes((flat[0][rows], flat[1][rows]), col_count))
    matrix = lambda i, j: sums["image", min(i, j), max(i, j)]

    zero = jnp.zeros((col_count, slots), jnp.float32)
    nothing = (zero, zero)
    unit = (zero + 1.0, zero)
    number = lambda value: (zero + value, zero)
    inverses, factors, directions, shares = [], {}, [], []
    kept_last = None
    for k in range(ITERS):
        scaled = {}
        for j in range(k):
            value = matrix(k, j)
            for i in range(j):
                value = sub(value, mul(scaled[i], factors[j, i]))
            scaled[j] = value
            factors[k, j] = mul(value, inverses[j])
        target = sums["source", 0, k]
        for j in range(k):
            target = sub(target, mul(factors[k, j], shares[j][0]))
        removed = nothing
        for j in range(k):
            removed = tidy(add(removed, mul(scaled[j], factors[k, j])))
        direction = [nothing] * k + [unit]
        for j in range(k):
            for i in range(j + 1):
                direction[i] = sub(direction[i], mul(factors[k, j], directions[j][i]))
        directions.append(direction)
        if k < last:
            pivot = sub(matrix(k, k), removed)
            inverses.append(inverse(pivot))
            shares.append((target, mul(target, inverses[k])))
        else:
            kept_last = (target, removed)

    def applied(direction):
        count = len(direction)
        padded = direction + [nothing, nothing]
        out = []
        for i in range(count + 1):
            value = mul(padded[i], number(1.0 - CENTRE))
            if i:
                value = sub(value, mul(padded[i - 1], number(HALF if i == 1 else HALF / 2)))
            out.append(sub(value, mul(padded[i + 1], number(HALF / 2))))
        return out

    def combined(coefficients, row):
        return tree([value[0] * vectors[i, row] for i, value in enumerate(coefficients)], jnp.add)

    solution = [nothing] * ITERS
    remainder = [unit] + [nothing] * ITERS
    peak_rows = []

    def largest(rows):
        peak = tree([jnp.abs(one) for one in rows], jnp.maximum)
        return jnp.max(jnp.max(peak, axis=0, keepdims=True), axis=1, keepdims=True)

    for k in range(last):
        share = shares[k][1]
        image = applied(directions[k])
        for i, value in enumerate(directions[k]):
            solution[i] = tidy(add(solution[i], mul(share, value)))
        for i, value in enumerate(image):
            remainder[i] = sub(remainder[i], mul(share, value))
        rows = [diag_ref[row] * combined(remainder[: k + 2], row) for row in range(row_count)]
        peak_rows.append(largest(rows))
    residual_rows = rows
    image = applied(directions[last])
    solution_rows = [combined(solution[:last], row) for row in range(row_count)]
    direction_rows = [combined(directions[last], row) for row in range(row_count)]
    image_rows = [diag_ref[row] * combined(image, row) for row in range(row_count)]

    end_all(*late_args)
    pair = tree(
        [(gather_late[device, 0:1], gather_late[device, 1:2]) for device in range(device_count)], add
    )
    target, removed = kept_last
    pivot = sub(tidy(pair), (removed[0][0:1], removed[1][0:1]))
    share = target[0][0:1] / pivot[0]
    for row in range(row_count):
        residual_rows[row] = residual_rows[row] - share * image_rows[row]
        residual_ref[row] = residual_rows[row]
        pressure_ref[row] = solution_rows[row] + share * direction_rows[row]
    peak_rows.append(largest(residual_rows))
    lane = lax.broadcasted_iota(jnp.int32, (1, slots), 1)
    packed = jnp.zeros((1, slots), jnp.float32)
    for k in range(ITERS):
        packed = jnp.where(lane == k, peak_rows[k], packed)
    gather_peak[0] = packed
    start_all(*peak_args)

    end_sends(*field_args)
    end_sends(*density_args)
    end_sends(*deep_places_args)
    end_sends(*deep_density_args)
    for step in range(ITERS):
        if step - 1 not in DEEP:
            end_sends(*vector_args(step))
    end_all_sends(*early_args)
    end_all_sends(*late_args)
    end_all(*peak_args)
    peaks_ref[...] = tree([gather_peak[device] for device in range(device_count)], jnp.maximum)
    end_all_sends(*peak_args)


def write_out(density_ref, pressure_ref, residual_ref, peaks_ref, *rest):
    outs, packed_ref, sems = rest[:4], rest[4], rest[5]
    packed_ref[...] = peaks_ref[0, : packed_ref.shape[0]]
    copies = [
        pltpu.make_async_copy(source, target, sems.at[index])
        for index, (source, target) in enumerate(
            zip((density_ref, pressure_ref, residual_ref, packed_ref), outs)
        )
    ]
    for copy in copies:
        copy.start()
    for copy in copies:
        copy.wait()


def body(size_x, size_y, offsets, masses, counts, source):
    row_count, col_count, slots = masses.shape
    devices = size_x * size_y
    padded = (row_count + 2, col_count + 2)
    deep = (row_count + 4, col_count + 4)
    ring_count = padded[0] * padded[1] - row_count * col_count
    block = (row_count, col_count, slots)
    dma, f32, sides = pltpu.SemaphoreType.DMA, jnp.float32, len(SIDES)
    scratch = lambda *shape: pltpu.VMEM(shape, f32)
    group = slots // col_count
    early_rows = 2 * (-(-((ITERS - 1) * (ITERS + 2) // 2 - 1) // group) + -(-(ITERS + 1) // group))
    weight_bytes = 4 * row_count * col_count * len(NEIGHBOUR_STEPS) * slots * slots
    vmem = pl.BlockSpec(memory_space=pltpu.VMEM)
    hbm = pl.BlockSpec(memory_space=pltpu.HBM)
    shaped = jax.ShapeDtypeStruct(block, f32)
    results = pl.pallas_call(
        functools.partial(kernel, size_x, size_y, row_count, col_count),
        out_shape=(shaped, shaped, shaped, jax.ShapeDtypeStruct((1, slots), f32)),
        in_specs=[hbm] * 4,
        out_specs=(vmem,) * 4,
        scratch_shapes=[
            scratch(2, *block), scratch(*block), pltpu.VMEM((row_count, col_count), jnp.int32),
            scratch(*block), dma((4,)),
            scratch(*padded, 4, slots), scratch(*padded, 1, slots), scratch(ITERS, *deep, 1, slots),
            scratch(row_count, col_count, len(NEIGHBOUR_STEPS), slots, slots),
            scratch(row_count, col_count, slots, slots),
            scratch(row_count, col_count, slots, slots),
            scratch(row_count, col_count, slots, slots),
            scratch(row_count, col_count, 1, slots),
            scratch(row_count, col_count, 1, slots),
            scratch(*block),
            scratch(ITERS + 1, *block), scratch(ITERS, *block), scratch(ITERS, *block),
            scratch(*deep, 2, slots), scratch(*deep, 1, slots),
            scratch(ring_count, len(NEIGHBOUR_STEPS), slots, slots), scratch(ring_count, 1, slots),
            scratch(ring_count, 1, slots), scratch(ring_count, 3, slots, slots),
            scratch(devices, early_rows, slots), scratch(devices, 2, slots), scratch(devices, 1, slots),
            dma((sides,)), dma((sides,)), dma((sides,)), dma((sides,)),
            dma((ITERS, sides)), dma((ITERS, sides)),
            dma((devices,)), dma((devices,)), dma((devices,)), dma((devices,)),
            dma((devices,)), dma((devices,)),
            dma((sides,)), dma((sides,)), dma((sides,)), dma((sides,)),
        ],
        compiler_params=pltpu.CompilerParams(
            collective_id=0, has_side_effects=True, vmem_limit_bytes=4 * weight_bytes
        ),
    )(*(pltpu.with_memory_space_constraint(one, pltpu.HBM) for one in (offsets, masses, counts, source)))
    return pl.pallas_call(
        write_out,
        out_shape=(shaped, shaped, shaped, jax.ShapeDtypeStruct((ITERS,), f32)),
        in_specs=[vmem] * 4,
        out_specs=(hbm,) * 4,
        scratch_shapes=[scratch(ITERS), dma((4,))],
        compiler_params=pltpu.CompilerParams(vmem_limit_bytes=weight_bytes),
    )(*results)


def solution(mesh):
    in_specs = (P(None, "gx", "gy", None), P("gx", "gy", None), P("gx", "gy"), P("gx", "gy", None))
    out_specs = (P("gx", "gy", None), P("gx", "gy", None), P("gx", "gy", None), P())
    return jax.shard_map(
        functools.partial(body, mesh.shape["gx"], mesh.shape["gy"]),
        mesh=mesh, in_specs=in_specs, out_specs=out_specs, check_vma=False,
    )
```

```python
import functools

import jax
import jax.numpy as jnp
from jax import lax
from jax.experimental import pallas as pl
from jax.experimental.pallas import tpu as pltpu
from jax.sharding import PartitionSpec as P

ITERS = 5
BASE_STIFF = 0.5
PAIR_SCALE = 0.05
NEIGHBOUR_STEPS = [(step_x, step_y) for step_x in (-1, 0, 1) for step_y in (-1, 0, 1)]
SIDES = [step for step in NEIGHBOUR_STEPS if step != (0, 0)]
MESH = pl.DeviceIdType.MESH
FAR = 64.0
NODES, SCALE = (0.0, 0.875, 0.4375, 0.1875, 0.6875), 0.5
CHUNK = 64
DEEP = (1, 3)
SHORT_WAY, LONG_WAY = "short", "long"
READY = 9
FIRST = 13
MIDDLE = 0.5


def two_sum(a, b):
    total = a + b
    part = total - a
    return total, (a - (total - part)) + (b - part)


def add(a, b):
    high, low = two_sum(a[0], b[0])
    return high, low + (a[1] + b[1])


def tidy(a):
    high = a[0] + a[1]
    return high, a[1] - (high - a[0])


def halves(a):
    wide = a * 4097.0
    high = wide - (wide - a)
    return high, a - high


def mul(a, b):
    a_high, a_low = halves(a[0])
    b_high, b_low = halves(b[0])
    product = a[0] * b[0]
    rest = ((a_high * b_high - product) + (a_high * b_low + a_low * b_high)) + a_low * b_low
    return tidy((product, rest + (a[0] * b[1] + a[1] * b[0])))


def neg(a):
    return -a[0], -a[1]


def sub(a, b):
    return tidy(add(a, neg(b)))


def inverse(a):
    first = 1.0 / a[0]
    start = (first, jnp.zeros_like(first))
    one = (jnp.ones_like(first), jnp.zeros_like(first))
    rest = sub(one, mul(start, a))
    return tidy((first, rest[0] * first))


def tree(items, combine):
    items = list(items)
    while len(items) > 1:
        paired = [combine(items[at], items[at + 1]) for at in range(0, len(items) - 1, 2)]
        items = paired + items[len(paired) * 2 :]
    return items[0]


def over_sublanes(pair, rows):
    shift = rows // 2
    while shift:
        pair = add(pair, tuple(pltpu.roll(part, shift, 0) for part in pair))
        shift //= 2
    return pair


def kernel(
    size_x, size_y, row_count, col_count,
    offsets_hbm, masses_hbm, counts_hbm, source_hbm,
    density_ref, pressure_ref, residual_ref, peaks_ref,
    offsets_ref, masses_ref, counts_ref, source_ref, load_sem,
    pad_fields, pad_density, pad_vector, weights, own_x, own_y, own_density,
    part, inverse_diag, diag_ref, vectors, products, images,
    deep_places, deep_density, ring_weights, ring_inverse, ring_part, ring_own,
    gather_early, gather_late, gather_peak,
    field_send, field_recv, density_send, density_recv, vector_send, vector_recv,
    early_send, early_recv, late_send, late_recv, peak_send, peak_recv,
    deep_places_send, deep_places_recv, deep_density_send, deep_density_recv,
):
    here_x, here_y = lax.axis_index("gx"), lax.axis_index("gy")
    device_count = size_x * size_y
    slots = masses_ref.shape[-1]

    loads = [
        pltpu.make_async_copy(source, target, load_sem.at[index])
        for index, (source, target) in enumerate((
            (offsets_hbm, offsets_ref), (masses_hbm, masses_ref),
            (counts_hbm, counts_ref), (source_hbm, source_ref),
        ))
    ]
    for load in loads:
        load.start()

    low_x, high_x = (here_x > 0), (here_x < size_x - 1)
    low_y, high_y = (here_y > 0), (here_y < size_y - 1)

    def on_side(step_x, step_y, action):
        conditions = []
        if step_x:
            conditions.append({1: high_x, -1: low_x}[step_x])
        if step_y:
            conditions.append({1: high_y, -1: low_y}[step_y])
        condition = conditions[0]
        for other in conditions[1:]:
            condition = jnp.logical_and(condition, other)
        pl.when(condition)(action)

    def ahead(here, step, size):
        there = here + step
        return jnp.where(there >= size, there - size, there)

    def for_peers(action):
        def turned(step_y):
            return jnp.where(here_y < size_y // 2, size_y - step_y, step_y)

        if device_count <= 64:
            for step_y in range(1, size_y):
                for step_x in range(size_x - 1, -1, -1):
                    action(step_x * size_y + turned(step_y), step_x, turned(step_y))
            for step_x in range(1, size_x):
                action(step_x * size_y, step_x, 0)
        else:
            def one(index, carry):
                action(index, lax.div(index, size_y), lax.rem(index, size_y))
                return carry

            lax.fori_loop(1, device_count, one, 0)

    barrier = pltpu.get_barrier_semaphore()

    def greet(device):
        pl.semaphore_signal(barrier, inc=1, device_id=device, device_id_type=MESH)

    near_only = size_x <= ITERS + 2 and size_y <= ITERS + 3
    if near_only:
        for step_x, step_y in SIDES:
            on_side(step_x, step_y, functools.partial(greet, (here_x + step_x, here_y + step_y)))
        pl.when(here_y > 1)(lambda: greet((here_x, here_y - 2)))
        pl.when(here_y < size_y - 2)(lambda: greet((here_x, here_y + 2)))
    else:
        for_peers(lambda index, step_x, step_y: greet(
            (ahead(here_x, step_x, size_x), ahead(here_y, step_y, size_y))
        ))

    def fill(ref, value):
        ref[...] = jnp.full(ref.shape, value, jnp.float32)

    def fill_outside(axis, start):
        def at(margin):
            span = pl.ds(start + margin if start > 0 else 0, margin)
            return (span, slice(None)) if axis == 0 else (slice(None), span)

        fill(pad_fields.at[at(1)], FAR)
        fill(pad_density.at[at(1)], 1.0)
        fill(deep_places.at[at(2)], FAR)
        fill(deep_density.at[at(2)], 1.0)
        for step in range(ITERS):
            fill(pad_vector.at[(step,) + at(2)], 0.0)

    pl.when(jnp.logical_not(low_x))(lambda: fill_outside(0, 0))
    pl.when(jnp.logical_not(high_x))(lambda: fill_outside(0, row_count))
    pl.when(jnp.logical_not(low_y))(lambda: fill_outside(1, 0))
    pl.when(jnp.logical_not(high_y))(lambda: fill_outside(1, col_count))

    def halo_copy(side, pad, depth, send_sem, recv_sem):
        step_x, step_y = SIDES[side]
        margin = (pad.shape[0] - row_count) // 2

        def inner(step, count):
            start = margin + count - depth if step > 0 else margin
            return pl.ds(start, depth if step else count)

        def outer(step, count):
            start = {1: margin - depth, -1: margin + count, 0: margin}[step]
            return pl.ds(start, depth if step else count)

        return pltpu.make_async_remote_copy(
            src_ref=pad.at[inner(step_x, row_count), inner(step_y, col_count)],
            dst_ref=pad.at[outer(step_x, row_count), outer(step_y, col_count)],
            send_sem=send_sem.at[side],
            recv_sem=recv_sem.at[side],
            device_id=(here_x + step_x, here_y + step_y),
            device_id_type=MESH,
        )

    LONG = [side for side, step in enumerate(SIDES) if step[1]]
    SHORT = [side for side, step in enumerate(SIDES) if not step[1]]

    def start_halo(sides, *args):
        for side in sides:
            on_side(*SIDES[side], lambda side=side: halo_copy(side, *args).start())

    def end_halo(*args, sides=range(len(SIDES))):
        for side in sides:
            step_x, step_y = SIDES[side]
            on_side(-step_x, -step_y, lambda side=side: halo_copy(side, *args).wait_recv())

    def end_sends(*args):
        for side, (step_x, step_y) in enumerate(SIDES):
            on_side(step_x, step_y, lambda side=side: halo_copy(side, *args).wait_send())

    def steps_of(row, place, inside):
        def is_inside(step_x, step_y):
            if not 0 <= row + step_x < row_count:
                return False
            return not (place == "first" and step_y < 0 or place == "last" and step_y > 0)

        def is_wanted(step_x, step_y):
            if inside in (SHORT_WAY, LONG_WAY):
                long_way = place == "first" and step_y < 0 or place == "last" and step_y > 0
                return not is_inside(step_x, step_y) and long_way == (inside == LONG_WAY)
            return inside is None or is_inside(step_x, step_y) == inside

        return [
            (index, step_x, step_y)
            for index, (step_x, step_y) in enumerate(NEIGHBOUR_STEPS)
            if is_wanted(step_x, step_y)
        ]

    def columns(action, chosen):
        for col in chosen:
            place = "first" if col == 0 else "last" if col == col_count - 1 else "inner"
            for row in range(row_count):
                action(row, col, place)

    def edge_columns(action, depth=1):
        columns(action, [col for col in range(col_count) if not depth <= col < col_count - depth])

    def inner_columns(action, depth=1):
        columns(action, range(depth, col_count - depth))

    def all_columns(action):
        edge_columns(action)
        inner_columns(action)

    def spread(row):
        return jnp.broadcast_to(row, (slots, slots)).T

    def gathered(total):
        return jnp.sum(total.T, axis=0, keepdims=True)

    def chunks(terms):
        return gathered(jnp.concatenate(
            [terms(pl.ds(start, CHUNK)) for start in range(0, slots, CHUNK)], axis=0
        ))

    wide = col_count + 2
    ring = [(col + 1, -1, col) for col in range(-1, col_count + 1)]
    ring += [(wide + col + 1, row_count, col) for col in range(-1, col_count + 1)]
    ring += [(2 * wide + 2 * row, row, -1) for row in range(row_count)]
    ring += [(2 * wide + 2 * row + 1, row, col_count) for row in range(row_count)]

    ring_middle = [cell for cell in ring if 3 <= cell[2] < col_count - 3]
    ring_ends = [cell for cell in ring if cell not in ring_middle]
    ring_short = [
        cell for cell in ring if cell[1] in (-1, row_count) and 1 <= cell[2] < col_count - 1
    ]
    ring_long = [cell for cell in ring if cell not in ring_short]
    ring_at = {(row, col): at for at, row, col in ring}

    def known(at, row, col):
        out = []
        for index, (step_x, step_y) in enumerate(NEIGHBOUR_STEPS):
            cell = (row + step_x, col + step_y)
            back = len(NEIGHBOUR_STEPS) - 1 - index
            if 0 <= cell[0] < row_count and 0 <= cell[1] < col_count:
                out.append(("own", cell, back))
            elif cell in ring_at and order[ring_at[cell]] < order[at]:
                out.append(("ring", ring_at[cell], back))
            else:
                out.append(None)
        return out

    order = {at: place for place, (at, _, _) in enumerate(ring)}

    def spread_ring_places(at, row, col):
        places = deep_places[row + 2, col + 2]
        ring_own[at, 0] = spread(2.0 * places[0:1])
        ring_own[at, 1] = spread(2.0 * places[1:2])

    def spread_ring(at, row, col):
        if order[at] >= READY:
            spread_ring_places(at, row, col)
        ring_own[at, 2] = spread(deep_density[row + 2, col + 2])

    def in_turn(prepare, action, cells):
        prepare(*cells[0])
        for place, cell in enumerate(cells):
            if place + 1 < len(cells):
                prepare(*cells[place + 1])
            action(*cell)

    def ring_squares(at, row, col, rows):
        twice_x, twice_y = ring_own[at, 0, rows], ring_own[at, 1, rows]
        rest = 1.0 - 0.25 * (twice_x * twice_x + twice_y * twice_y)

        def one(index):
            step_x, step_y = NEIGHBOUR_STEPS[index]
            near = deep_places[row + 2 + step_x, col + 2 + step_y]
            near_x, near_y = near[0:1] + step_x, near[1:2] + step_y
            near_rest = near_x * near_x + near_y * near_y
            falloff = (rest - near_rest) + (twice_x * near_x + twice_y * near_y)
            falloff = jnp.maximum(falloff, 0.0)
            return falloff * falloff

        return one

    def parts():
        return [slice(start, start + CHUNK) for start in range(0, slots, CHUNK)]

    def set_ring_squares(at, row, col):
        for rows in parts():
            squares = ring_squares(at, row, col, rows)
            for index, found in enumerate(known(at, row, col)):
                if found is None:
                    ring_weights[at, index, rows] = squares(index)

    def set_ring_weights(at, row, col):
        ready = order[at] < READY
        totals = []
        turned = {}
        for index, found in enumerate(known(at, row, col)):
            if found is None:
                continue
            kind, cell, back = found
            if kind == "own":
                turned[index] = weights[cell[0], cell[1], back].T
                places = deep_places[cell[0] + 2, cell[1] + 2]
                live = (places[0:1] < FAR / 2).astype(jnp.float32)
            else:
                turned[index] = ring_weights[cell, back].T
                live = 1.0
            ring_weights[at, index] = turned[index]
            turned[index] = turned[index] * live
        for rows in parts():
            squares = None if ready else ring_squares(at, row, col, rows)
            here = ring_own[at, 2, rows]
            total = None
            for index, (step_x, step_y) in enumerate(NEIGHBOUR_STEPS):
                if index in turned:
                    weight = turned[index][rows]
                else:
                    there = deep_density[row + 2 + step_x, col + 2 + step_y]
                    square = ring_weights[at, index, rows] if ready else squares(index)
                    weight = square / (here + there)
                    ring_weights[at, index, rows] = weight
                total = weight if total is None else total + weight
            totals.append(total)
        total = gathered(jnp.concatenate(totals, axis=0))
        live = (deep_places[row + 2, col + 2][0:1] < FAR / 2).astype(jnp.float32)
        ring_inverse[at] = live / (BASE_STIFF + live * total)

    def set_ring_share(step):
        if step > DEEP[0]:
            return
        if step == 0:
            end_halo(*deep_density_args)
        share = ring[:FIRST] if step == 0 else ring[FIRST:]
        in_turn(spread_ring, set_ring_weights, share)

    def ring_product(step, at, row, col, inside):
        total = None
        for index, (step_x, step_y) in enumerate(NEIGHBOUR_STEPS):
            own = 0 <= row + step_x < row_count and 0 <= col + step_y < col_count
            if inside is None or own == inside:
                term = ring_weights[at, index] * pad_vector[step, row + 2 + step_x, col + 2 + step_y]
                total = term if total is None else total + term
        return gathered(total)

    def start_ring(step):
        if step == DEEP[1]:
            for at, row, col in ring:
                ring_part[at] = ring_product(step, at, row, col, True)

    def finish_ring(step, cells):
        for at, row, col in cells:
            if step == DEEP[1]:
                product = ring_part[at] + ring_product(step, at, row, col, False)
            else:
                product = ring_product(step, at, row, col, None)
            rest = ring_inverse[at] * product - NODES[step] * pad_vector[step, row + 2, col + 2]
            following = rest * (1.0 / SCALE)
            pad_vector[step + 1, row + 2, col + 2] = following

    for load in loads:
        load.wait()
    lane = lax.broadcasted_iota(jnp.int32, (col_count, slots), 1)
    square = (col_count, col_count)
    on_diagonal = lax.broadcasted_iota(jnp.int32, square, 0) == lax.broadcasted_iota(jnp.int32, square, 1)
    occupied = []
    for row in range(row_count):
        limits = jnp.where(
            on_diagonal, jnp.broadcast_to(counts_ref[row : row + 1].astype(jnp.float32), square), 0.0
        )
        limit = jnp.sum(limits, axis=1, keepdims=True)
        occupied.append((lane.astype(jnp.float32) < limit).astype(jnp.float32))
        live = occupied[row] > 0.0
        field_rows = (
            jnp.where(live, offsets_ref[0, row], FAR),
            jnp.where(live, offsets_ref[1, row], FAR),
            masses_ref[row],
            source_ref[row] * occupied[row],
        )
        source_ref[row] = field_rows[3]
        for col in range(col_count):
            for index in range(3):
                pad_fields[row + 1, col + 1, index : index + 1] = field_rows[index][col : col + 1]
            for index in range(2):
                centred = field_rows[index][col : col + 1] - MIDDLE
                deep_places[row + 2, col + 2, index : index + 1] = centred
        inverse_diag[row] = occupied[row].reshape(col_count, 1, slots)

    greeters = lambda low, high: low.astype(jnp.int32) + high.astype(jnp.int32)
    if near_only:
        count_x, count_y = greeters(low_x, high_x), greeters(low_y, high_y)
        further = greeters(here_y > 1, here_y < size_y - 2)
        pl.semaphore_wait(barrier, (count_x + 1) * (count_y + 1) - 1 + further)
    else:
        pl.semaphore_wait(barrier, device_count - 1)

    field_args = (pad_fields, 1, field_send, field_recv)
    start_halo(range(len(SIDES)), *field_args)
    deep_places_args = (deep_places, 2, deep_places_send, deep_places_recv)
    start_halo(range(len(SIDES)), *deep_places_args)

    def spread_place(row, col, place):
        own_x[row, col] = spread(offsets_ref[0, row, pl.ds(col, 1)])
        own_y[row, col] = spread(offsets_ref[1, row, pl.ds(col, 1)])

    all_columns(spread_place)

    def density_part(inside):
        def one(row, col, place):
            steps = steps_of(row, place, inside)

            def terms(rows):
                at_x, at_y = own_x[row, col, rows], own_y[row, col, rows]
                total = None
                for index, step_x, step_y in steps:
                    near = pad_fields[row + 1 + step_x, col + 1 + step_y]
                    offset_x = (step_x + near[0:1]) - at_x
                    offset_y = (step_y + near[1:2]) - at_y
                    falloff = jnp.maximum(1.0 - (offset_x * offset_x + offset_y * offset_y), 0.0)
                    squared = falloff * falloff
                    weights[row, col, index, rows] = squared
                    term = squared * falloff * near[2:3]
                    total = term if total is None else total + term
                return total

            return chunks(terms)

        return one

    def store_density_part(row, col, place):
        part[row, col] = density_part(True)(row, col, place)

    def add_density_part(row, col, place):
        part[row, col] = part[row, col] + density_part(SHORT_WAY)(row, col, place)

    all_columns(store_density_part)
    end_halo(*field_args, sides=SHORT)
    edge_columns(add_density_part)
    end_halo(*field_args, sides=LONG)

    def finish_density(row, col, place):
        rest = density_part(False if place == "inner" else LONG_WAY)(row, col, place)
        density = 1.0 + (part[row, col] + rest)
        pad_density[row + 1, col + 1] = density
        deep_density[row + 2, col + 2] = density * (0.5 / PAIR_SCALE)
        density_ref[row, pl.ds(col, 1)] = density

    density_args = (pad_density, 1, density_send, density_recv)
    deep_density_args = (deep_density, 2, deep_density_send, deep_density_recv)
    edge_columns(finish_density)
    start_halo(LONG, *density_args)
    inner_columns(finish_density)
    start_halo(SHORT, *density_args)
    start_halo(range(len(SIDES)), *deep_density_args)

    def weight_part(inside):
        def one(row, col, place):
            steps = steps_of(row, place, inside)

            def terms(rows):
                here = own_density[row, col, rows]
                total = None
                for index, step_x, step_y in steps:
                    there = pad_density[row + 1 + step_x, col + 1 + step_y]
                    weight = weights[row, col, index, rows] * ((2.0 * PAIR_SCALE) / (here + there))
                    weights[row, col, index, rows] = weight
                    total = weight if total is None else total + weight
                return total

            return chunks(terms)

        return one

    def store_weight_part(row, col, place):
        own_density[row, col] = spread(pad_density[row + 1, col + 1])
        part[row, col] = weight_part(True)(row, col, place)

    all_columns(store_weight_part)
    end_halo(*deep_places_args)
    in_turn(spread_ring_places, set_ring_squares, ring[:READY])
    end_halo(*density_args)

    def finish_weights(row, col, place):
        occupied_row = inverse_diag[row, col]
        total = part[row, col] + weight_part(False)(row, col, place)
        diagonal = BASE_STIFF + occupied_row * total
        inverted = occupied_row / diagonal
        scaled = source_ref[row, pl.ds(col, 1)] * inverted
        diag_ref[row, pl.ds(col, 1)] = diagonal
        inverse_diag[row, col] = inverted
        vectors[0, row, pl.ds(col, 1)] = scaled
        pad_vector[0, row + 2, col + 2] = scaled

    def vector_args(step):
        depth = 2 if step in DEEP else 1
        return pad_vector.at[step], depth, vector_send.at[step], vector_recv.at[step]

    edge_columns(finish_weights)
    start_halo(LONG, *vector_args(0))
    inner_columns(finish_weights)
    start_halo(SHORT, *vector_args(0))

    def product_part(step, inside):
        def one(row, col, place):
            total = None
            for index, step_x, step_y in steps_of(row, place, inside):
                term = weights[row, col, index] * pad_vector[step, row + 2 + step_x, col + 2 + step_y]
                total = term if total is None else total + term
            return gathered(total)

        return one

    def store_product_part(step):
        def one(row, col, place):
            part[row, col] = product_part(step, True)(row, col, place)

        return one

    def finish_product(step):
        def one(row, col, place):
            if step - 1 in DEEP:
                product = product_part(step, None)(row, col, place)
            else:
                product = part[row, col] + product_part(step, False)(row, col, place)
            products[step, row, pl.ds(col, 1)] = product
            now = vectors[step, row, pl.ds(col, 1)]
            following = (inverse_diag[row, col] * product - NODES[step] * now) * (1.0 / SCALE)
            vectors[step + 1, row, pl.ds(col, 1)] = following
            if step + 1 < ITERS:
                pad_vector[step + 1, row + 2, col + 2] = following

        return one

    def set_image(step):
        for row in range(row_count):
            images[step, row] = diag_ref[row] * vectors[step, row] - products[step, row]

    def dot(left, right):
        zero = jnp.zeros((col_count, slots), jnp.float32)
        return tree([(left[row] * right[row], zero) for row in range(row_count)], add)

    def send_all(gather, send_sem, recv_sem):
        def one(index, step_x, step_y):
            return pltpu.make_async_remote_copy(
                src_ref=gather.at[0],
                dst_ref=gather.at[index],
                send_sem=send_sem.at[index],
                recv_sem=recv_sem.at[index],
                device_id=(ahead(here_x, step_x, size_x), ahead(here_y, step_y, size_y)),
                device_id_type=MESH,
            )

        return one

    def start_all(*args):
        for_peers(lambda *peer: send_all(*args)(*peer).start())

    def end_all(*args):
        for_peers(lambda *peer: send_all(*args)(*peer).wait_recv())

    def end_all_sends(*args):
        for_peers(lambda *peer: send_all(*args)(*peer).wait_send())

    early_args = (gather_early, early_send, early_recv)
    late_args = (gather_late, late_send, late_recv)
    peak_args = (gather_peak, peak_send, peak_recv)
    last = ITERS - 1
    group = slots // col_count
    entries = [("image", i, j) for j in range(last) for i in range(min(j + 1, last - 1))]
    entries += [("source", 0, j) for j in range(last)]
    late_entries = [("image", last - 1, last - 1), ("source", 0, last)]
    late_entries += [("image", i, last) for i in range(last)]
    entries += [None] * (-len(entries) % group) + late_entries
    groups = -(-len(entries) // group)
    first_late = groups - -(-len(late_entries) // group)

    def early_sums(chosen):
        filler = jnp.zeros((col_count, slots), jnp.float32)
        for at in chosen:
            rows = []
            for entry in entries[at * group : (at + 1) * group]:
                if entry is None:
                    rows.append((filler, filler))
                    continue
                kind, i, j = entry
                rows.append(dot(images.at[i] if kind == "image" else source_ref, vectors.at[j]))
            rows = rows + [(filler, filler)] * (group - len(rows))
            flat = [jnp.concatenate([pair[which] for pair in rows], axis=0).T for which in (0, 1)]
            slabs = [
                (flat[0][start : start + 8], flat[1][start : start + 8]) for start in range(0, slots, 8)
            ]
            pair = over_sublanes(tree(slabs, add), 8)
            gather_early[0, at : at + 1] = pair[0][0:1]
            gather_early[0, groups + at : groups + at + 1] = pair[1][0:1]

    def sum_lanes(pair):
        flat = [jnp.broadcast_to(part_of[0:1], (slots, slots)).T for part_of in pair]
        slabs = [(flat[0][start : start + 8], flat[1][start : start + 8]) for start in range(0, slots, 8)]
        return over_sublanes(tree(slabs, add), 8)

    def end_product(step):
        sends = step < last and step not in DEEP
        depth = 2 if step + 1 in DEEP else 1
        if step == DEEP[1]:
            inner_columns(finish_product(step), depth)
            finish_ring(step, ring_short)
            end_halo(*vector_args(step), sides=LONG)
        edge_columns(finish_product(step), depth)
        if sends:
            start_halo(LONG, *vector_args(step + 1))
        if step - 1 in DEEP and sends:
            finish_ring(step - 1, ring_middle)
        if step != DEEP[1]:
            inner_columns(finish_product(step), depth)
        if sends:
            start_halo(SHORT, *vector_args(step + 1))
        if step < last:
            set_image(step)

    for step in range(last):
        if step - 1 not in DEEP:
            all_columns(store_product_part(step))
            set_ring_share(step)
            if step == DEEP[1]:
                early_sums(range(first_late))
            start_ring(step)
            if step == DEEP[1]:
                end_halo(*vector_args(step), sides=SHORT)
            else:
                end_halo(*vector_args(step))
        end_product(step)
        if step == last - 1:
            early_sums(range(first_late, groups))
            start_all(*early_args)
        if step in DEEP:
            finish_ring(step, ring_ends if step == DEEP[0] else ring_long)

    crossing = []
    for row in range(row_count):
        for col in range(col_count):
            place = "first" if col == 0 else "last" if col == col_count - 1 else "inner"
            inside = [index for index, _, _ in steps_of(row, place, True)]
            single = twice = None
            for index, (step_x, step_y) in enumerate(NEIGHBOUR_STEPS):
                if index in inside and (step_x, step_y) < (0, 0):
                    continue
                term = weights[row, col, index] * pad_vector[last, row + 2 + step_x, col + 2 + step_y]
                if index in inside and (step_x, step_y) > (0, 0):
                    twice = term if twice is None else twice + term
                else:
                    single = term if single is None else single + term
            total = single if twice is None else single + (twice + twice)
            total = total * spread(vectors[last, row, pl.ds(col, 1)])
            crossing.append(tree([total[start : start + 8] for start in range(0, slots, 8)], jnp.add))
    zero = jnp.zeros((8, slots), jnp.float32)
    pair = tree([(-one, zero) for one in crossing], add)
    for row in range(row_count):
        now = vectors[last, row]
        pair = add(pair, (diag_ref[row] * now * now, zero))
    pair = sum_lanes(over_sublanes(pair, 8))
    gather_late[0, 0:1] = pair[0][0:1]
    gather_late[0, 1:2] = pair[1][0:1]
    start_all(*late_args)

    end_product(last)
    end_all(*early_args)
    sums = {}
    for at in range(groups):
        pair = tree(
            [
                (gather_early[device, at : at + 1], gather_early[device, groups + at : groups + at + 1])
                for device in range(device_count)
            ],
            add,
        )
        flat = [spread(part_of) for part_of in pair]
        for index, entry in enumerate(entries[at * group : (at + 1) * group]):
            if entry is None:
                continue
            rows = slice(index * col_count, (index + 1) * col_count)
            sums[entry] = tidy(over_sublanes((flat[0][rows], flat[1][rows]), col_count))
    matrix = lambda i, j: sums["image", min(i, j), max(i, j)]

    zero = jnp.zeros((col_count, slots), jnp.float32)
    nothing = (zero, zero)
    unit = (zero + 1.0, zero)
    number = lambda value: (zero + value, zero)
    inverses, factors, directions, shares = [], {}, [], []
    kept_last = None
    for k in range(ITERS):
        scaled = {}
        for j in range(k):
            value = matrix(k, j)
            for i in range(j):
                value = sub(value, mul(scaled[i], factors[j, i]))
            scaled[j] = value
            factors[k, j] = mul(value, inverses[j])
        target = sums["source", 0, k]
        for j in range(k):
            target = sub(target, mul(factors[k, j], shares[j][0]))
        removed = nothing
        for j in range(k):
            removed = tidy(add(removed, mul(scaled[j], factors[k, j])))
        direction = [nothing] * k + [unit]
        for j in range(k):
            for i in range(j + 1):
                direction[i] = sub(direction[i], mul(factors[k, j], directions[j][i]))
        directions.append(direction)
        if k < last:
            pivot = sub(matrix(k, k), removed)
            inverses.append(inverse(pivot))
            shares.append((target, mul(target, inverses[k])))
        else:
            kept_last = (target, removed)

    def applied(direction):
        count = len(direction)
        out = [mul(value, number(1.0 - NODES[i])) for i, value in enumerate(direction)] + [nothing]
        for i in range(count):
            out[i + 1] = sub(out[i + 1], mul(direction[i], number(SCALE)))
        return out

    def combined(coefficients, row):
        return tree([value[0] * vectors[i, row] for i, value in enumerate(coefficients)], jnp.add)

    solution = [nothing] * ITERS
    remainder = [unit] + [nothing] * ITERS
    peak_rows = []

    def largest(rows):
        peak = tree([jnp.abs(one) for one in rows], jnp.maximum)
        return jnp.max(jnp.max(peak, axis=0, keepdims=True), axis=1, keepdims=True)

    for k in range(last):
        share = shares[k][1]
        image = applied(directions[k])
        for i, value in enumerate(directions[k]):
            solution[i] = tidy(add(solution[i], mul(share, value)))
        for i, value in enumerate(image):
            remainder[i] = sub(remainder[i], mul(share, value))
        rows = [diag_ref[row] * combined(remainder[: k + 2], row) for row in range(row_count)]
        peak_rows.append(largest(rows))
    residual_rows = rows
    image = applied(directions[last])
    solution_rows = [combined(solution[:last], row) for row in range(row_count)]
    direction_rows = [combined(directions[last], row) for row in range(row_count)]
    image_rows = [diag_ref[row] * combined(image, row) for row in range(row_count)]

    end_all(*late_args)
    pair = tree(
        [(gather_late[device, 0:1], gather_late[device, 1:2]) for device in range(device_count)], add
    )
    target, removed = kept_last
    pivot = sub(tidy(pair), (removed[0][0:1], removed[1][0:1]))
    share = target[0][0:1] / pivot[0]
    for row in range(row_count):
        residual_rows[row] = residual_rows[row] - share * image_rows[row]
        residual_ref[row] = residual_rows[row]
        pressure_ref[row] = solution_rows[row] + share * direction_rows[row]
    peak_rows.append(largest(residual_rows))
    lane = lax.broadcasted_iota(jnp.int32, (1, slots), 1)
    packed = jnp.zeros((1, slots), jnp.float32)
    for k in range(ITERS):
        packed = jnp.where(lane == k, peak_rows[k], packed)
    gather_peak[0] = packed
    start_all(*peak_args)

    end_sends(*field_args)
    end_sends(*density_args)
    end_sends(*deep_places_args)
    end_sends(*deep_density_args)
    for step in range(ITERS):
        if step - 1 not in DEEP:
            end_sends(*vector_args(step))
    end_all_sends(*early_args)
    end_all_sends(*late_args)
    end_all(*peak_args)
    peaks_ref[...] = tree([gather_peak[device] for device in range(device_count)], jnp.maximum)
    end_all_sends(*peak_args)


def write_out(density_ref, pressure_ref, residual_ref, peaks_ref, *rest):
    outs, packed_ref, sems = rest[:4], rest[4], rest[5]
    packed_ref[...] = peaks_ref[0, : packed_ref.shape[0]]
    copies = [
        pltpu.make_async_copy(source, target, sems.at[index])
        for index, (source, target) in enumerate(
            zip((density_ref, pressure_ref, residual_ref, packed_ref), outs)
        )
    ]
    for copy in copies:
        copy.start()
    for copy in copies:
        copy.wait()


def body(size_x, size_y, offsets, masses, counts, source):
    row_count, col_count, slots = masses.shape
    devices = size_x * size_y
    padded = (row_count + 2, col_count + 2)
    deep = (row_count + 4, col_count + 4)
    ring_count = padded[0] * padded[1] - row_count * col_count
    block = (row_count, col_count, slots)
    dma, f32, sides = pltpu.SemaphoreType.DMA, jnp.float32, len(SIDES)
    scratch = lambda *shape: pltpu.VMEM(shape, f32)
    group = slots // col_count
    early_rows = 2 * (-(-((ITERS - 1) * (ITERS + 2) // 2 - 1) // group) + -(-(ITERS + 1) // group))
    weight_bytes = 4 * row_count * col_count * len(NEIGHBOUR_STEPS) * slots * slots
    vmem = pl.BlockSpec(memory_space=pltpu.VMEM)
    hbm = pl.BlockSpec(memory_space=pltpu.HBM)
    shaped = jax.ShapeDtypeStruct(block, f32)
    results = pl.pallas_call(
        functools.partial(kernel, size_x, size_y, row_count, col_count),
        out_shape=(shaped, shaped, shaped, jax.ShapeDtypeStruct((1, slots), f32)),
        in_specs=[hbm] * 4,
        out_specs=(vmem,) * 4,
        scratch_shapes=[
            scratch(2, *block), scratch(*block), pltpu.VMEM((row_count, col_count), jnp.int32),
            scratch(*block), dma((4,)),
            scratch(*padded, 4, slots), scratch(*padded, 1, slots), scratch(ITERS, *deep, 1, slots),
            scratch(row_count, col_count, len(NEIGHBOUR_STEPS), slots, slots),
            scratch(row_count, col_count, slots, slots),
            scratch(row_count, col_count, slots, slots),
            scratch(row_count, col_count, slots, slots),
            scratch(row_count, col_count, 1, slots),
            scratch(row_count, col_count, 1, slots),
            scratch(*block),
            scratch(ITERS + 1, *block), scratch(ITERS, *block), scratch(ITERS, *block),
            scratch(*deep, 2, slots), scratch(*deep, 1, slots),
            scratch(ring_count, len(NEIGHBOUR_STEPS), slots, slots), scratch(ring_count, 1, slots),
            scratch(ring_count, 1, slots), scratch(ring_count, 3, slots, slots),
            scratch(devices, early_rows, slots), scratch(devices, 2, slots), scratch(devices, 1, slots),
            dma((sides,)), dma((sides,)), dma((sides,)), dma((sides,)),
            dma((ITERS, sides)), dma((ITERS, sides)),
            dma((devices,)), dma((devices,)), dma((devices,)), dma((devices,)),
            dma((devices,)), dma((devices,)),
            dma((sides,)), dma((sides,)), dma((sides,)), dma((sides,)),
        ],
        compiler_params=pltpu.CompilerParams(
            collective_id=0, has_side_effects=True, vmem_limit_bytes=4 * weight_bytes
        ),
    )(*(pltpu.with_memory_space_constraint(one, pltpu.HBM) for one in (offsets, masses, counts, source)))
    return pl.pallas_call(
        write_out,
        out_shape=(shaped, shaped, shaped, jax.ShapeDtypeStruct((ITERS,), f32)),
        in_specs=[vmem] * 4,
        out_specs=(hbm,) * 4,
        scratch_shapes=[scratch(ITERS), dma((4,))],
        compiler_params=pltpu.CompilerParams(vmem_limit_bytes=weight_bytes),
    )(*results)


def solution(mesh):
    in_specs = (P(None, "gx", "gy", None), P("gx", "gy", None), P("gx", "gy"), P("gx", "gy", None))
    out_specs = (P("gx", "gy", None), P("gx", "gy", None), P("gx", "gy", None), P())
    return jax.shard_map(
        functools.partial(body, mesh.shape["gx"], mesh.shape["gy"]),
        mesh=mesh, in_specs=in_specs, out_specs=out_specs, check_vma=False,
    )
```
